32 devices in a mesh: kgrp: 4 (over x, core), tile: 8 (over z, y).
Axes of the slice: x: 2, y: 2, z: 4, core: 2. Of those that a mesh axis runs over, the one named last changes fastest.
Arguments:
- mask_spectrum: float32 [32, 2, 512, 512], P(('kgrp', 'tile')), may hold values from -6 to 6
- kernels: float32 [8, 2, 512, 512], P('kgrp', None, 'tile'), may hold values from -6 to 6
- owner_table: int32 [4], replicated, may hold values from 0 to 7
- step_weight: float32 [4], replicated, may hold values from 0.25 to 1
Outputs:
- intensity: float32 [32, 512, 512], P(('kgrp', 'tile'))
The draws below stay inside these ranges and needn't reach their ends.
Inputs may be any that keep to these rules, and one draw needn't show every extreme that they name: `owner_table`: kernel indices, possibly repeated across steps.
All inputs are finite; a program needn't handle non-finite values.
Results may differ from the reference program's by a relative error of at most 0.0001.
Values sent between devices are 32-bit elements; how exact they have to be, the bound alone decides.
A program may use at most 128 MiB of HBM per device.

```python
import math
import jax
import jax.numpy as jnp

KS = 512
STEPS = 4
KERNELS = 8
TILES = 32


def with_ends(entries, rng, least, high):
    longest = entries.shape.index(max(entries.shape))
    spots = []
    for shift in (0, 1):
        where = [jax.random.randint(jax.random.fold_in(rng, axis), (), 0, length) for axis, length in enumerate(entries.shape)]
        where[longest] = (where[longest] + shift) % entries.shape[longest]
        spots.append(tuple(where))
    return entries.at[spots[0]].set(least).at[spots[1]].set(high)


def shard_levels(rng, shape, cuts, least, largest):
    level = 1.0
    for position, parts in cuts:
        draws = jax.random.uniform(jax.random.fold_in(jax.random.fold_in(rng, 6), position), (parts,), jnp.float32, least / len(cuts), largest / len(cuts))
        level = level * jnp.repeat(jnp.exp(draws), shape[position] // parts).reshape((-1,) + (1,) * (len(shape) - 1 - position))
    return level


def bell_draw(own_key, shape, deviation, reach, pieces=(), kind=jnp.bfloat16):
    entries = deviation * jax.random.normal(own_key, shape, jnp.float32)
    if pieces:
        entries = entries * shard_levels(own_key, shape, pieces, -0.22, 0.18)
    return jnp.clip(entries, -reach, reach).astype(kind)


def setup_inputs(seed: int = 0) -> dict:
    key_of = jax.random.split(jax.random.key(seed), 5)
    mask_spectrum = bell_draw(key_of[0], (TILES, 2, KS, KS), 0.7, 6.0, ((0, 32),), jnp.float32)
    kernels = bell_draw(key_of[1], (KERNELS, 2, KS, KS), 0.7, 6.0, ((0, 4), (2, 8)), jnp.float32)
    owner_table = with_ends(jax.random.randint(key_of[2], (STEPS,), 0, KERNELS), jax.random.fold_in(key_of[2], 1), 0, KERNELS - 1).astype(jnp.int32)
    step_weight = jnp.clip(jnp.exp(jax.random.uniform(key_of[3], (STEPS,), jnp.float32, math.log(0.25), math.log(1.0))), 0.25, 1.0)
    return {"mask_spectrum": mask_spectrum, "kernels": kernels, "owner_table": owner_table, "step_weight": step_weight}


def reference(mask_spectrum, kernels, owner_table, step_weight):
    mask_field = mask_spectrum[:, 0] + 1j * mask_spectrum[:, 1]
    intensity = jnp.zeros_like(mask_spectrum[:, 0])
    for step in range(STEPS):
        kernel_pick = kernels[owner_table[step]]
        spectrum = mask_field * (kernel_pick[0] + 1j * kernel_pick[1])[None]
        aerial_field = jnp.fft.ifft2(spectrum, norm="ortho")
        power = jnp.real(aerial_field) ** 2 + jnp.imag(aerial_field) ** 2
        intensity = intensity + step_weight[step] * power.astype(intensity.dtype)
    return intensity
```

```python
import functools
import math

import jax
import jax.numpy as jnp
import ml_dtypes
import numpy as np
from jax import lax
from jax.experimental import pallas as pl
from jax.experimental.pallas import tpu as pltpu
from jax.sharding import PartitionSpec as P

MESH = pl.DeviceIdType.MESH
BF = jnp.bfloat16
F32 = jnp.float32


def split_np(x):
    hi = x.astype(np.float32).astype(ml_dtypes.bfloat16)
    lo = (x - hi.astype(np.float64)).astype(np.float32).astype(ml_dtypes.bfloat16)
    return hi, lo


def tables(n, radix):
    m = n // radix
    a = np.arange(m)
    rows = []
    for r in range(radix):
        phase = (a[:, None] * (r + radix * a[None, :])) % n * (2.0 * math.pi / n)
        c, s = np.cos(phase) / math.sqrt(n), np.sin(phase) / math.sqrt(n)
        rows.append(np.block([[c, s], [-s, c]]))
    b = np.stack(rows)
    bh, bl = split_np(b)
    row = np.concatenate([bh, bl], axis=1)
    col = np.concatenate([bh.transpose(0, 2, 1), bl.transpose(0, 2, 1)], axis=2)
    return row, col


def split(x):
    hi = x.astype(BF)
    return hi, (x - hi.astype(F32)).astype(BF)


def radix4(re, im):
    ar, ai, br, bi = re[0] + re[2], im[0] + im[2], re[0] - re[2], im[0] - im[2]
    cr, ci, dr, di = re[1] + re[3], im[1] + im[3], re[1] - re[3], im[1] - im[3]
    return [(ar + cr, ai + ci), (br - di, bi + dr), (ar - cr, ai - ci), (br + di, bi - dr)]


OWN, Z_IN, Y_IN, ACROSS, ROWS, COLUMNS = range(6)
TUNED = {
    (2, 4, 4, 3, 4): [
        (0, 0, 0), (0, 0, 1), (0, 0, 2), (1, 0, 1, 0), (0, 1, 0), (1, 0, 1, 1), (1, 0, 2, 0), (0, 0, 3),
        (2, 0, 1, 0), (1, 0, 1, 2), (1, 0, 2, 1), (1, 0, 3, 0), (1, 0, 2, 2), (0, 1, 1), (4, 0, 2, 0), (2, 0, 0, 0),
        (4, 0, 1, 0), (4, 0, 0, 0), (1, 1, 1, 0), (2, 0, 2, 0), (2, 0, 0, 1), (2, 1, 0, 0), (1, 0, 3, 1), (0, 1, 2),
        (1, 0, 3, 2), (1, 1, 1, 1), (2, 0, 1, 1), (4, 0, 3, 0), (2, 0, 3, 0), (2, 0, 0, 2), (4, 0, 0, 1), (2, 0, 3, 1),
        (1, 1, 2, 0), (1, 1, 1, 2), (0, 1, 3), (2, 0, 2, 1), (2, 0, 1, 2), (3, 1, 0), (4, 1, 0, 0), (1, 1, 3, 0),
        (2, 0, 2, 2), (4, 1, 1, 0), (4, 0, 2, 1), (2, 0, 3, 2), (4, 0, 3, 1), (1, 1, 2, 1), (2, 1, 0, 1), (1, 1, 2, 2),
        (3, 1, 1), (2, 1, 0, 2), (4, 0, 1, 1), (3, 1, 2), (2, 1, 1, 0), (4, 1, 2, 0), (5, 0, 1, 0), (2, 1, 2, 0),
        (5, 0, 1, 1), (1, 1, 3, 1), (4, 1, 0, 1), (5, 0, 1, 2), (5, 0, 1, 3), (2, 1, 2, 1), (2, 1, 3, 0), (1, 1, 3, 2),
        (5, 0, 0, 0), (5, 0, 0, 1), (2, 1, 1, 1), (5, 0, 0, 2), (4, 1, 3, 0), (2, 1, 3, 1), (2, 1, 2, 2), (5, 0, 0, 3),
        (2, 1, 1, 2), (4, 1, 1, 1), (4, 1, 2, 1), (2, 1, 3, 2), (4, 1, 3, 1), (5, 1, 1, 0), (5, 1, 1, 1), (5, 1, 1, 2),
        (5, 1, 1, 3), (5, 1, 0, 0), (5, 1, 0, 1), (5, 1, 0, 2), (5, 1, 0, 3),
    ],
}


def program(spc, nz, pieces, parts, radix):
    key = (spc, nz, pieces, len(parts), radix)
    if key in TUNED:
        return TUNED[key]
    order = []
    for l in range(spc):
        order += [(OWN, l, p) for p in range(pieces)]
        end = l == spc - 1
        for j in range(nz):
            order += [(Z_IN, l, j, p) for p in parts if j]
            order += [(Y_IN, l, j, p) for p in parts if not (end and j == 1)]
        order += [(ACROSS, l, p) for p in parts if end]
        order += [(Y_IN, l, 1, p) for p in parts if end]
        order += [(ROWS, l, k, other) for k in range(nz) for other in (0, 1)]
        order += [(COLUMNS, l, tile, rx) for tile in (1, 0) for rx in range(radix)]
    return order


def kernel(dims, owner_ref, weight_ref, mask_hbm, kern_hbm, rowt_hbm, colt_hbm, out_ref,
           kern, side, held, mask, rowt, colt, lane_perm, stage, field, cols, total, part, blocks,
           loc, k_send, k_recv, m_send, m_recv, e_send, e_recv, up_send, down_send, relay_send, z_recv,
           y_send, y_recv, across_up, across_down, x_send, x_recv, p_send, p_recv):
    spc, nk, nz, rows, n, radix = dims
    m = n // radix
    last = spc - 1
    g = lax.axis_index("kgrp")
    t = lax.axis_index("tile")
    x, c = g // 2, g % 2
    z, y = t // 2, t % 2
    xo, co, yo = 1 - x, 1 - c, 1 - y
    x_peer, c_peer = {"kgrp": 2 * xo + c}, {"kgrp": 2 * x + co}
    y_peer = {"tile": 2 * z + yo}

    def at_z(i):
        return {"tile": 2 * i + y}

    unit = 8
    nt = rows // unit
    share = nt // 4
    keep = nt - share
    wide = max(share, 1)
    cuts = [(i, i + wide) for i in range(0, nt, wide)]
    parts = [p for p, cut in enumerate(cuts) if cut[1] <= keep]

    def span(s, p):
        a, b = cuts[p]
        return pl.ds(pl.multiple_of(a * unit + s * (rows - unit * (a + b)), unit), unit * (b - a))

    own_kern = kern.at[pl.ds(c * nk, nk)]
    loads = [
        pltpu.make_async_copy(kern_hbm, own_kern, loc.at[0]),
        pltpu.make_async_copy(mask_hbm, mask.at[0], loc.at[1]),
        pltpu.make_async_copy(rowt_hbm, rowt, loc.at[2]),
        pltpu.make_async_copy(colt_hbm, colt, loc.at[3]),
    ]
    for load in loads:
        load.start()

    barrier = pltpu.get_barrier_semaphore()
    for peer in (c_peer, x_peer, y_peer):
        pl.semaphore_signal(barrier, inc=1, device_id=peer, device_id_type=MESH)

    @pl.when(z > 0)
    def _():
        pl.semaphore_signal(barrier, inc=1, device_id=at_z(z - 1), device_id_type=MESH)

    @pl.when(z < nz - 1)
    def _():
        pl.semaphore_signal(barrier, inc=1, device_id=at_z(z + 1), device_id_type=MESH)

    src_lane = lax.broadcasted_iota(jnp.int32, (n, n), 0)
    dst_lane = lax.broadcasted_iota(jnp.int32, (n, n), 1)
    lane_perm[...] = jnp.where((src_lane % m) * radix + src_lane // m == dst_lane, 1.0, 0.0).astype(BF)
    loads[0].wait()

    pl.semaphore_wait(barrier, 3 + jnp.minimum(z, 1) + jnp.minimum(nz - 1 - z, 1))

    sent = []

    def send(src, dst, send_sem, recv_sem, device, cond=None):
        copy = pltpu.make_async_remote_copy(src_ref=src, dst_ref=dst, send_sem=send_sem, recv_sem=recv_sem,
                                            device_id=device, device_id_type=MESH)
        if cond is None:
            copy.start()
        else:
            pl.when(cond)(copy.start)
        sent.append((copy, cond))

    def arrive(ref, recv_sem):
        pltpu.make_async_remote_copy(src_ref=ref, dst_ref=ref, send_sem=recv_sem, recv_sem=recv_sem,
                                     device_id=c_peer, device_id_type=MESH).wait_recv()

    def piece(l, zz, yy, s, p):
        return held.at[l, zz, yy, :, span(s, p)]

    for p in range(len(cuts)):
        src = kern.at[pl.ds(c * nk, nk), :, span(xo, p)]
        send(src, src, k_send.at[p], k_recv.at[p], c_peer)
    send(mask_hbm, mask.at[1], m_send.at[0], m_recv.at[0], c_peer)

    owners = [owner_ref[c * spc + l] for l in range(spc)]
    for p in range(len(cuts)):
        arrive(kern.at[pl.ds(co * nk, nk), :, span(xo, p)], k_recv.at[p])
    for l in range(spc):
        for p in range(len(cuts)):
            side[x, l, :, span(xo, p)] = kern[owners[l] % (2 * nk), :, span(xo, p)]
    for l in range(spc):
        for p in range(len(cuts)):
            src = side.at[x, l, :, span(xo, p)]
            send(src, src, e_send.at[l, p], e_recv.at[l, p], x_peer)

    def own(l, p):
        arrive(side.at[xo, l, :, span(x, p)], e_recv.at[l, p])
        mine = owners[l] // (2 * nk) == x
        held[l, z, y, :, span(x, p)] = jnp.where(mine, side[x, l, :, span(x, p)], side[xo, l, :, span(x, p)])
        if p in parts:
            here = piece(l, z, y, x, p)
            send(here, here, y_send.at[l, z, p], y_recv.at[l, z, p], y_peer)
            send(here, here, down_send.at[l, p], z_recv.at[l, z, p], at_z(z - 1), z > 0)
            send(here, here, up_send.at[l, p], z_recv.at[l, z, p], at_z(z + 1), z < nz - 1)

    def across(l, p):
        here = piece(l, z, yo, x, p)
        send(here, here, across_down.at[p], y_recv.at[l, z, p], at_z(z - 1), z > 0)
        send(here, here, across_up.at[p], y_recv.at[l, z, p], at_z(z + 1), z < nz - 1)

    def share_x(l, zz, yy, cond=None):
        if share:
            here = piece(l, zz, yy, x, 0)
            send(here, here, x_send.at[l, zz, yy], x_recv.at[l, zz, yy], x_peer, cond)

    def z_in(l, j, p):
        for zz, have, dest, more in ((z + j, z + j < nz, z - 1, z > 0), (z - j, z >= j, z + 1, z < nz - 1)):
            here = piece(l, zz, y, x, p)
            pl.when(have)(functools.partial(arrive, here, z_recv.at[l, zz, p]))
            if j < nz - 1:
                send(here, here, relay_send.at[l, zz, p], z_recv.at[l, zz, p], at_z(dest), have & more)
            if l != last or j > 1:
                send(here, here, y_send.at[l, zz, p], y_recv.at[l, zz, p], y_peer, have)
            if p == 0:
                share_x(l, zz, y, have)

    def y_in(l, j, p):
        if j == 0:
            arrive(piece(l, z, yo, x, p), y_recv.at[l, z, p])
            if p == 0:
                share_x(l, z, yo)
            return
        for zz, have in ((z + j, z + j < nz), (z - j, z >= j)):
            pl.when(have)(functools.partial(arrive, piece(l, zz, yo, x, p), y_recv.at[l, zz, p]))
            if p == 0:
                share_x(l, zz, yo, have)

    def near(k):
        if k == 0:
            return z
        low = jnp.minimum(z, nz - 1 - z)
        both = z + (k + 1) // 2 if k % 2 else z - k // 2
        one = jnp.where(low == z, z + k - low, z - k + low)
        return jnp.where(k <= 2 * low, both, one)

    def x_in(l, k, yy):
        if share and not (k == 0 and yy is y):
            arrive(piece(l, near(k), yy, xo, 0), x_recv.at[l, near(k), yy])

    def rows_in(l, blocks_in):
        for j, (k, yy) in enumerate(blocks_in):
            zi = near(k)
            i = 2 * zi + yy
            at = pl.ds(pl.multiple_of(i * rows, rows), rows)

            @pl.loop(0, 2)
            def _(tile):
                to = pl.ds(pl.multiple_of((2 * j + tile) * rows, rows), rows)
                re, im = [], []
                for q in range(radix):
                    kr, ki = held[l, zi, yy, 0, :, q * m:(q + 1) * m], held[l, zi, yy, 1, :, q * m:(q + 1) * m]
                    mr, mi = mask[tile, 0, at, q * m:(q + 1) * m], mask[tile, 1, at, q * m:(q + 1) * m]
                    re.append(mr * kr - mi * ki)
                    im.append(mr * ki + mi * kr)
                for r, (pr, pi) in enumerate(radix4(re, im)):
                    for p, v in enumerate((pr, pi)):
                        hi, lo = split(v)
                        stage[r, to, p * m:(p + 1) * m] = hi
                        stage[r, to, (2 + p) * m:(3 + p) * m] = lo

        size = 2 * len(blocks_in) * rows
        for r in range(radix):
            hi, lo = stage[r, :size, :2 * m], stage[r, :size, 2 * m:]
            th, tl = rowt[r, :2 * m], rowt[r, 2 * m:]
            done = jnp.dot(jnp.concatenate([hi, lo, hi], 1), jnp.concatenate([th, th, tl], 0),
                           preferred_element_type=F32)
            for j, (k, yy) in enumerate(blocks_in):
                i = 2 * near(k) + yy
                for tile in range(2):
                    field[l, r, tile, pl.ds(pl.multiple_of(i * rows, rows), rows)] = (
                        done[(2 * j + tile) * rows:(2 * j + tile + 1) * rows])

    half = m // 4

    def middle(l, tile):
        for ry in range(radix):
            @pl.loop(0, 4)
            def _(i):
                base = pl.multiple_of(i * half, half)
                re = [field[l, ry, tile, pl.ds(k * m + base, half), :m] for k in range(radix)]
                im = [field[l, ry, tile, pl.ds(k * m + base, half), m:] for k in range(radix)]
                for rx, pair in enumerate(radix4(re, im)):
                    for p, v in enumerate(pair):
                        hi, lo = split(v)
                        cols[rx, pl.ds(p * m + base, half), ry * m:(ry + 1) * m] = hi
                        cols[rx, pl.ds((2 + p) * m + base, half), ry * m:(ry + 1) * m] = lo

    def columns(l, tile, rx):
        hi, lo = cols[rx, :2 * m], cols[rx, 2 * m:]
        th, tl = colt[rx, :, :2 * m], colt[rx, :, 2 * m:]
        done = jnp.dot(jnp.concatenate([th, th, tl], 1), jnp.concatenate([hi, lo, hi], 0),
                       preferred_element_type=F32)
        power = (done[:m] * done[:m] + done[m:] * done[m:]) * weight_ref[c * spc + l]
        if l == 0:
            total[tile, rx] = power
        else:
            total[tile, rx] += power

    def row_step(l, k, other):
        yy = yo if other else y
        x_in(l, k, yy)
        rows_in(l, [(k, yy)])

    def column_step(l, tile, rx):
        if rx == 0:
            middle(l, tile)
        columns(l, tile, rx)
        if l == last and tile == 1:
            for done in [rx - 1] if rx < radix - 1 else [rx - 1, rx]:
                if done >= 0:
                    send(total.at[1, done], part.at[done], p_send.at[done], p_recv.at[done], c_peer)

    steps = (own, z_in, y_in, across, row_step, column_step)
    first_row = True
    for op, *args in program(spc, nz, len(cuts), parts, radix):
        if op == 4 and first_row:
            first_row = False
            for load in loads[1:]:
                load.wait()
            arrive(mask.at[1], m_recv.at[0])
        steps[op](*args)

    for rx in range(radix):
        arrive(part.at[rx], p_recv.at[rx])
        hi, lo = split(total[0, rx] + part[rx])
        perm = lane_perm[...]
        image = jnp.dot(jnp.concatenate([hi, lo], 1), jnp.concatenate([perm, perm], 0), preferred_element_type=F32)
        for q in range(radix):
            blocks[q, pl.ds(rx, m, stride=radix), :] = image[:, q * m:(q + 1) * m]
    for q in range(radix):
        out_ref[:, q * m:(q + 1) * m] = blocks[q]
    for copy, cond in sent:
        if cond is None:
            copy.wait_send()
        else:
            pl.when(cond)(copy.wait_send)


def local(mesh_shape, mask_spectrum, kernels, owner_table, step_weight):
    groups, tiles = mesh_shape
    nk, _, rows, n = kernels.shape
    steps = owner_table.shape[0]
    radix = 4
    m = n // radix
    spc = steps // 2
    nz = tiles // 2
    most = rows // 8
    rowt, colt = tables(n, radix)
    dma = pltpu.SemaphoreType.DMA
    any_spec = pl.BlockSpec(memory_space=pl.ANY)
    smem = pl.BlockSpec(memory_space=pltpu.SMEM)
    out = pl.pallas_call(
        functools.partial(kernel, (spc, nk, nz, rows, n, radix)),
        out_shape=jax.ShapeDtypeStruct((n, n), F32),
        in_specs=[smem, smem, any_spec, any_spec, any_spec, any_spec],
        out_specs=pl.BlockSpec(memory_space=pltpu.VMEM),
        scratch_shapes=[
            pltpu.VMEM((2 * nk, 2, rows, n), F32),
            pltpu.VMEM((2, spc, 2, rows, n), F32),
            pltpu.VMEM((spc, nz, 2, 2, rows, n), F32),
            pltpu.VMEM((2, 2, n, n), F32),
            pltpu.VMEM(rowt.shape, BF),
            pltpu.VMEM(colt.shape, BF),
            pltpu.VMEM((n, n), BF),
            pltpu.VMEM((radix, 4 * rows, 4 * m), BF),
            pltpu.VMEM((spc, radix, 2, n, 2 * m), F32),
            pltpu.VMEM((radix, 4 * m, n), BF),
            pltpu.VMEM((2, radix, m, n), F32),
            pltpu.VMEM((radix, m, n), F32),
            pltpu.VMEM((radix, n, m), F32),
            dma((4,)), dma((most,)), dma((most,)), dma((1,)), dma((1,)), dma((spc, most)), dma((spc, most)),
            dma((spc, most)), dma((spc, most)), dma((spc, nz, most)), dma((spc, nz, most)),
            dma((spc, nz, most)), dma((spc, nz, most)), dma((most,)), dma((most,)),
            dma((spc, nz, 2)), dma((spc, nz, 2)), dma((radix,)), dma((radix,)),
        ],
        compiler_params=pltpu.CompilerParams(collective_id=0, has_side_effects=True, vmem_limit_bytes=54 * 1024 * 1024),
    )(owner_table, step_weight, mask_spectrum[0], kernels, jnp.asarray(rowt), jnp.asarray(colt))
    return out[None]


def solution(mesh):
    in_specs = (P(("kgrp", "tile"), None, None, None), P("kgrp", None, "tile", None), P(), P())
    out_specs = P(("kgrp", "tile"), None, None)
    body = functools.partial(local, (mesh.shape["kgrp"], mesh.shape["tile"]))
    return jax.shard_map(body, mesh=mesh, in_specs=in_specs, out_specs=out_specs, check_vma=False)
```

```python
import functools
import math

import jax
import jax.numpy as jnp
import ml_dtypes
import numpy as np
from jax import lax
from jax.experimental import pallas as pl
from jax.experimental.pallas import tpu as pltpu
from jax.sharding import PartitionSpec as P

MESH = pl.DeviceIdType.MESH
BF = jnp.bfloat16
F32 = jnp.float32


def split_np(x):
    hi = x.astype(np.float32).astype(ml_dtypes.bfloat16)
    lo = (x - hi.astype(np.float64)).astype(np.float32).astype(ml_dtypes.bfloat16)
    return hi, lo


def tables(n, radix):
    m = n // radix
    a = np.arange(m)
    rows = []
    for r in range(radix):
        phase = (a[:, None] * (r + radix * a[None, :])) % n * (2.0 * math.pi / n)
        c, s = np.cos(phase) / math.sqrt(n), np.sin(phase) / math.sqrt(n)
        rows.append(np.block([[c, s], [-s, c]]))
    b = np.stack(rows)
    bh, bl = split_np(b)
    row = np.concatenate([bh, bl], axis=1)
    col = np.concatenate([bh.transpose(0, 2, 1), bl.transpose(0, 2, 1)], axis=2)
    return row, col


def split(x):
    hi = x.astype(BF)
    return hi, (x - hi.astype(F32)).astype(BF)


def radix4(re, im):
    ar, ai, br, bi = re[0] + re[2], im[0] + im[2], re[0] - re[2], im[0] - im[2]
    cr, ci, dr, di = re[1] + re[3], im[1] + im[3], re[1] - re[3], im[1] - im[3]
    return [(ar + cr, ai + ci), (br - di, bi + dr), (ar - cr, ai - ci), (br + di, bi - dr)]


OWN, Z_IN, Y_IN, ACROSS, ROWS, COLUMNS = range(6)
TUNED = {
    (2, 4, 4, 3, 4): [
        (0, 0, 0), (0, 0, 1), (0, 0, 2), (1, 0, 1, 0), (0, 1, 0), (1, 0, 1, 1), (1, 0, 2, 0), (0, 0, 3),
        (2, 0, 1, 0), (1, 0, 1, 2), (1, 0, 2, 1), (1, 0, 3, 0), (1, 0, 2, 2), (0, 1, 1), (4, 0, 2, 0), (2, 0, 0, 0),
        (4, 0, 1, 0), (4, 0, 0, 0), (1, 1, 1, 0), (2, 0, 2, 0), (2, 0, 0, 1), (2, 1, 0, 0), (1, 0, 3, 1), (0, 1, 2),
        (1, 0, 3, 2), (1, 1, 1, 1), (2, 0, 1, 1), (4, 0, 3, 0), (2, 0, 3, 0), (2, 0, 0, 2), (4, 0, 0, 1), (2, 0, 3, 1),
        (1, 1, 2, 0), (1, 1, 1, 2), (0, 1, 3), (2, 0, 2, 1), (2, 0, 1, 2), (3, 1, 0), (4, 1, 0, 0), (1, 1, 3, 0),
        (2, 0, 2, 2), (4, 1, 1, 0), (4, 0, 2, 1), (2, 0, 3, 2), (4, 0, 3, 1), (1, 1, 2, 1), (2, 1, 0, 1), (1, 1, 2, 2),
        (3, 1, 1), (2, 1, 0, 2), (4, 0, 1, 1), (3, 1, 2), (2, 1, 1, 0), (4, 1, 2, 0), (5, 0, 1, 0), (2, 1, 2, 0),
        (5, 0, 1, 1), (1, 1, 3, 1), (4, 1, 0, 1), (5, 0, 1, 2), (5, 0, 1, 3), (2, 1, 2, 1), (2, 1, 3, 0), (1, 1, 3, 2),
        (5, 0, 0, 0), (5, 0, 0, 1), (2, 1, 1, 1), (5, 0, 0, 2), (4, 1, 3, 0), (2, 1, 3, 1), (2, 1, 2, 2), (5, 0, 0, 3),
        (2, 1, 1, 2), (4, 1, 1, 1), (4, 1, 2, 1), (2, 1, 3, 2), (4, 1, 3, 1), (5, 1, 1, 0), (5, 1, 1, 1), (5, 1, 1, 2),
        (5, 1, 1, 3), (5, 1, 0, 0), (5, 1, 0, 1), (5, 1, 0, 2), (5, 1, 0, 3),
    ],
}


def program(spc, nz, pieces, parts, radix):
    key = (spc, nz, pieces, len(parts), radix)
    if key in TUNED:
        return TUNED[key]
    order = []
    for l in range(spc):
        order += [(OWN, l, p) for p in range(pieces)]
        end = l == spc - 1
        for j in range(nz):
            order += [(Z_IN, l, j, p) for p in parts if j]
            order += [(Y_IN, l, j, p) for p in parts if not (end and j == 1)]
        order += [(ACROSS, l, p) for p in parts if end]
        order += [(Y_IN, l, 1, p) for p in parts if end]
        order += [(ROWS, l, k, other) for k in range(nz) for other in (0, 1)]
        order += [(COLUMNS, l, tile, rx) for tile in (1, 0) for rx in range(radix)]
    return order


def kernel(dims, owner_ref, weight_ref, mask_hbm, kern_hbm, rowt_hbm, colt_hbm, out_ref,
           kern, side, held, mask, rowt, colt, lane_perm, stage, field, cols, total, part, blocks,
           loc, k_recv, m_recv, e_recv, z_recv, y_recv, x_recv, p_recv, gone):
    spc, nk, nz, rows, n, radix = dims
    m = n // radix
    last = spc - 1
    g = lax.axis_index("kgrp")
    t = lax.axis_index("tile")
    x, c = g // 2, g % 2
    z, y = t // 2, t % 2
    xo, co, yo = 1 - x, 1 - c, 1 - y
    x_peer, c_peer = {"kgrp": 2 * xo + c}, {"kgrp": 2 * x + co}
    y_peer = {"tile": 2 * z + yo}

    def at_z(i):
        return {"tile": 2 * i + y}

    unit = 8
    nt = rows // unit
    share = nt // 4
    keep = nt - share
    wide = max(share, 1)
    cuts = [(i, i + wide) for i in range(0, nt, wide)]
    parts = [p for p, cut in enumerate(cuts) if cut[1] <= keep]

    def span(s, p):
        a, b = cuts[p]
        return pl.ds(pl.multiple_of(a * unit + s * (rows - unit * (a + b)), unit), unit * (b - a))

    barrier = pltpu.get_barrier_semaphore()
    for peer in (c_peer, x_peer, y_peer):
        pl.semaphore_signal(barrier, inc=1, device_id=peer, device_id_type=MESH)

    @pl.when(z > 0)
    def _():
        pl.semaphore_signal(barrier, inc=1, device_id=at_z(z - 1), device_id_type=MESH)

    @pl.when(z < nz - 1)
    def _():
        pl.semaphore_signal(barrier, inc=1, device_id=at_z(z + 1), device_id_type=MESH)

    own_kern = kern.at[pl.ds(c * nk, nk)]
    loads = [
        pltpu.make_async_copy(kern_hbm, own_kern, loc.at[0]),
        pltpu.make_async_copy(mask_hbm, mask.at[0], loc.at[1]),
        pltpu.make_async_copy(rowt_hbm, rowt, loc.at[2]),
        pltpu.make_async_copy(colt_hbm, colt, loc.at[3]),
    ]
    for load in loads:
        load.start()
    loads[0].wait()
    pl.semaphore_wait(barrier, 3 + jnp.minimum(z, 1) + jnp.minimum(nz - 1 - z, 1))

    groups = {}

    def send(src, dst, recv_sem, device, group, cond=None):
        index, _, size = groups.setdefault(group, (len(groups), cond, 0))
        groups[group] = index, cond, size + math.prod(src.shape) // n
        copy = pltpu.make_async_remote_copy(src_ref=src, dst_ref=dst, send_sem=gone.at[index], recv_sem=recv_sem,
                                            device_id=device, device_id_type=MESH)
        if cond is None:
            copy.start()
        else:
            pl.when(cond)(copy.start)

    def all_gone():
        for index, cond, size in groups.values():
            if size <= n:
                ref = mask.at[0, 0, pl.ds(0, size)]
            elif size <= 2 * n:
                ref = mask.at[0, :, pl.ds(0, size // 2)]
            else:
                ref = mask.at[:, :, pl.ds(0, size // 4)]
            wait = pltpu.make_async_remote_copy(src_ref=ref, dst_ref=ref, send_sem=gone.at[index],
                                                recv_sem=gone.at[index], device_id=c_peer, device_id_type=MESH).wait_send
            if cond is None:
                wait()
            else:
                pl.when(cond)(wait)

    def arrive(ref, recv_sem):
        pltpu.make_async_remote_copy(src_ref=ref, dst_ref=ref, send_sem=recv_sem, recv_sem=recv_sem,
                                     device_id=c_peer, device_id_type=MESH).wait_recv()

    def piece(l, zz, yy, s, p):
        return held.at[l, zz, yy, :, span(s, p)]

    for p in range(len(cuts)):
        src = kern.at[pl.ds(c * nk, nk), :, span(xo, p)]
        send(src, src, k_recv.at[p], c_peer, "core")
    send(mask_hbm, mask.at[1], m_recv.at[0], c_peer, "mask")

    owners = [owner_ref[c * spc + l] for l in range(spc)]
    for p in range(len(cuts)):
        arrive(kern.at[pl.ds(co * nk, nk), :, span(xo, p)], k_recv.at[p])
    for p in range(len(cuts)):
        for l in range(spc):
            side[x, l, :, span(xo, p)] = kern[owners[l] % (2 * nk), :, span(xo, p)]
        src = side.at[x, 0, :, span(xo, p)]
        send(src, src, e_recv.at[0, p], x_peer, "core")
    for l in range(1, spc):
        for p in range(len(cuts)):
            src = side.at[x, l, :, span(xo, p)]
            send(src, src, e_recv.at[l, p], x_peer, "core")

    half = n // 2
    wide_lane = m // 2
    src_lane = lax.broadcasted_iota(jnp.int32, (half, half), 0)
    dst_lane = lax.broadcasted_iota(jnp.int32, (half, half), 1)
    perm = jnp.where((src_lane % wide_lane) * radix + src_lane // wide_lane == dst_lane, 1.0, 0.0).astype(BF)
    lane_perm[:half] = perm
    lane_perm[half:] = perm

    def own(l, p):
        arrive(side.at[xo, l, :, span(x, p)], e_recv.at[l, p])
        mine = owners[l] // (2 * nk) == x
        held[l, z, y, :, span(x, p)] = jnp.where(mine, side[x, l, :, span(x, p)], side[xo, l, :, span(x, p)])
        if p in parts:
            here = piece(l, z, y, x, p)
            send(here, here, y_recv.at[l, z, p], y_peer, "core")
            send(here, here, z_recv.at[l, z, p], at_z(z - 1), "down", z > 0)
            send(here, here, z_recv.at[l, z, p], at_z(z + 1), "up", z < nz - 1)

    def across(l, p):
        here = piece(l, z, yo, x, p)
        send(here, here, y_recv.at[l, z, p], at_z(z - 1), "down", z > 0)
        send(here, here, y_recv.at[l, z, p], at_z(z + 1), "up", z < nz - 1)

    def share_x(l, zz, yy, group, cond=None):
        if share:
            here = piece(l, zz, yy, x, 0)
            send(here, here, x_recv.at[l, zz, yy], x_peer, group, cond)

    def z_in(l, j, p):
        for s, zz, have, dest, more in ((1, z + j, z + j < nz, z - 1, z > 0), (-1, z - j, z >= j, z + 1, z < nz - 1)):
            here = piece(l, zz, y, x, p)
            pl.when(have)(functools.partial(arrive, here, z_recv.at[l, zz, p]))
            if j < nz - 1:
                send(here, here, z_recv.at[l, zz, p], at_z(dest), ("relay", s * j), have & more)
            if l != last or j > 1:
                send(here, here, y_recv.at[l, zz, p], y_peer, ("on", s * j), have)
            if p == 0:
                share_x(l, zz, y, ("on", s * j), have)

    def y_in(l, j, p):
        if j == 0:
            arrive(piece(l, z, yo, x, p), y_recv.at[l, z, p])
            if p == 0:
                share_x(l, z, yo, "core")
            return
        for s, zz, have in ((1, z + j, z + j < nz), (-1, z - j, z >= j)):
            pl.when(have)(functools.partial(arrive, piece(l, zz, yo, x, p), y_recv.at[l, zz, p]))
            if p == 0:
                share_x(l, zz, yo, ("on", s * j), have)

    def near(k):
        if k == 0:
            return z
        low = jnp.minimum(z, nz - 1 - z)
        both = z + (k + 1) // 2 if k % 2 else z - k // 2
        one = jnp.where(low == z, z + k - low, z - k + low)
        return jnp.where(k <= 2 * low, both, one)

    def x_in(l, k, yy):
        if share and not (k == 0 and yy is y):
            arrive(piece(l, near(k), yy, xo, 0), x_recv.at[l, near(k), yy])

    strip = 16
    waiting = []
    ready = []

    def product(l, k, yy, slot, tile, strip_index):
        zi = near(k)
        lo_row = strip * strip_index
        at = pl.ds(pl.multiple_of((2 * zi + yy) * rows + lo_row, strip), strip)
        src = slice(lo_row, lo_row + strip)
        to = slice(tile * rows + lo_row, tile * rows + lo_row + strip)
        re, im = [], []
        for q in range(radix):
            lanes = slice(q * m, (q + 1) * m)
            kr, ki = held[l, zi, yy, 0, src, lanes], held[l, zi, yy, 1, src, lanes]
            mr, mi = mask[tile, 0, at, lanes], mask[tile, 1, at, lanes]
            re.append(mr * kr - mi * ki)
            im.append(mr * ki + mi * kr)
        for r, pair in enumerate(radix4(re, im)):
            for p, v in enumerate(pair):
                hi, lo = split(v)
                stage[slot, r, to, p * m:(p + 1) * m] = hi
                stage[slot, r, to, (2 + p) * m:(3 + p) * m] = lo

    def row_matmul(l, k, yy, slot, r):
        hi, lo = stage[slot, r, :, :2 * m], stage[slot, r, :, 2 * m:]
        th, tl = rowt[r, :2 * m], rowt[r, 2 * m:]
        done = jnp.dot(jnp.concatenate([hi, lo, hi], 1), jnp.concatenate([th, th, tl], 0),
                       preferred_element_type=F32)
        at = pl.ds(pl.multiple_of((2 * near(k) + yy) * rows, rows), rows)
        for tile in range(2):
            field[l, r, tile, at] = done[tile * rows:(tile + 1) * rows]

    def woven(first, second):
        count = max(len(first), len(second))
        for i in range(count):
            for group in (first, second):
                for work in group[i * len(group) // count:(i + 1) * len(group) // count]:
                    work()

    def held_matmuls():
        works = [functools.partial(row_matmul, *waiting[0], r) for r in range(radix)] if waiting else []
        waiting.clear()
        return works

    def row_step(l, k, other):
        yy = yo if other else y
        x_in(l, k, yy)
        slot = 1 - waiting[0][3] if waiting else 0
        products = [functools.partial(product, l, k, yy, slot, tile, i)
                    for i in range(rows // strip) for tile in range(2)]
        woven(held_matmuls(), products)
        waiting.append((l, k, yy, slot))

    def middle(l, tile, ry):
        def strip_of(i):
            base = i * strip
            lanes = slice(ry * m, (ry + 1) * m)
            re = [field[l, ry, tile, k * m + base:k * m + base + strip, :m] for k in range(radix)]
            im = [field[l, ry, tile, k * m + base:k * m + base + strip, m:] for k in range(radix)]
            for rx, pair in enumerate(radix4(re, im)):
                for p, v in enumerate(pair):
                    hi, lo = split(v)
                    cols[tile, rx, p * m + base:p * m + base + strip, lanes] = hi
                    cols[tile, rx, (2 + p) * m + base:(2 + p) * m + base + strip, lanes] = lo
        return [functools.partial(strip_of, i) for i in range(m // strip)]

    def columns(l, tile, rx):
        hi, lo = cols[tile, rx, :2 * m], cols[tile, rx, 2 * m:]
        th, tl = colt[rx, :, :2 * m], colt[rx, :, 2 * m:]
        done = jnp.dot(jnp.concatenate([th, th, tl], 1), jnp.concatenate([hi, lo, hi], 0),
                       preferred_element_type=F32)
        power = (done[:m] * done[:m] + done[m:] * done[m:]) * weight_ref[c * spc + l]
        if l == 0:
            total[tile, rx] = power
        else:
            total[tile, rx] += power

    def column_step(l, tile, rx):
        if rx == 0 and waiting and waiting[0][0] == l:
            woven(held_matmuls(), [])
        if rx == 0 and (l, tile) not in ready:
            for ry in range(radix):
                woven(middle(l, tile, ry), [])
        woven([functools.partial(columns, l, tile, rx)], middle(l, 1 - tile, rx) if tile == 1 else [])
        if tile == 1:
            ready.append((l, 0))
        if l == last and tile == 1:
            for done in [rx - 1] if rx < radix - 1 else [rx - 1, rx]:
                if done >= 0:
                    send(total.at[1, done], part.at[done], p_recv.at[0], c_peer, "part")

    steps = (own, z_in, y_in, across, row_step, column_step)
    first_row = True
    for op, *args in program(spc, nz, len(cuts), parts, radix):
        if op == 4 and first_row:
            first_row = False
            for load in loads[1:]:
                load.wait()
            arrive(mask.at[1], m_recv.at[0])
        steps[op](*args)

    arrive(part, p_recv.at[0])
    low = lax.broadcasted_iota(jnp.int32, (m, m), 1) < wide_lane
    perm = lane_perm[...]
    for rx in range(radix):
        lanes = [total[0, rx, :, r * m:(r + 1) * m] + part[rx, :, r * m:(r + 1) * m] for r in range(radix)]
        turned = [pltpu.roll(v, wide_lane, 1) for v in lanes]
        for h in range(2):
            pairs = [jnp.where(low, *((lanes[r], turned[r + 1]) if h == 0 else (turned[r], lanes[r + 1])))
                     for r in range(0, radix, 2)]
            hi, lo = split(jnp.concatenate(pairs, 1))
            image = jnp.dot(jnp.concatenate([hi, lo], 1), perm, preferred_element_type=F32)
            for q in range(radix // 2):
                blocks[h * (radix // 2) + q, pl.ds(rx, m, stride=radix), :] = image[:, q * m:(q + 1) * m]
    for q in range(radix):
        out_ref[:, q * m:(q + 1) * m] = blocks[q]
    all_gone()


def local(mesh_shape, mask_spectrum, kernels, owner_table, step_weight):
    groups, tiles = mesh_shape
    nk, _, rows, n = kernels.shape
    steps = owner_table.shape[0]
    radix = 4
    m = n // radix
    spc = steps // 2
    nz = tiles // 2
    most = min(rows // 8, 4)
    rowt, colt = tables(n, radix)
    dma = pltpu.SemaphoreType.DMA
    any_spec = pl.BlockSpec(memory_space=pl.ANY)
    smem = pl.BlockSpec(memory_space=pltpu.SMEM)
    out = pl.pallas_call(
        functools.partial(kernel, (spc, nk, nz, rows, n, radix)),
        out_shape=pltpu.VMEM((n, n), F32),
        in_specs=[smem, smem, any_spec, any_spec, any_spec, any_spec],
        out_specs=pl.BlockSpec(memory_space=pltpu.VMEM),
        scratch_shapes=[
            pltpu.VMEM((2 * nk, 2, rows, n), F32),
            pltpu.VMEM((2, spc, 2, rows, n), F32),
            pltpu.VMEM((spc, nz, 2, 2, rows, n), F32),
            pltpu.VMEM((2, 2, n, n), F32),
            pltpu.VMEM(rowt.shape, BF),
            pltpu.VMEM(colt.shape, BF),
            pltpu.VMEM((n, n // 2), BF),
            pltpu.VMEM((2, radix, 2 * rows, 4 * m), BF),
            pltpu.VMEM((spc, radix, 2, n, 2 * m), F32),
            pltpu.VMEM((2, radix, 4 * m, n), BF),
            pltpu.VMEM((2, radix, m, n), F32),
            pltpu.VMEM((radix, m, n), F32),
            pltpu.VMEM((radix, n, m), F32),
            dma((4,)), dma((most,)), dma((1,)), dma((spc, most)), dma((spc, nz, most)), dma((spc, nz, most)),
            dma((spc, nz, 2)), dma((1,)), dma((4 * nz + 2,)),
        ],
        compiler_params=pltpu.CompilerParams(collective_id=0, has_side_effects=True, vmem_limit_bytes=54 * 1024 * 1024),
    )(owner_table, step_weight, mask_spectrum[0], kernels, jnp.asarray(rowt), jnp.asarray(colt))
    return out[None]


def solution(mesh):
    in_specs = (P(("kgrp", "tile"), None, None, None), P("kgrp", None, "tile", None), P(), P())
    out_specs = P(("kgrp", "tile"), None, None)
    body = functools.partial(local, (mesh.shape["kgrp"], mesh.shape["tile"]))
    return jax.shard_map(body, mesh=mesh, in_specs=in_specs, out_specs=out_specs, check_vma=False)
```

```python
import functools
import math

import jax
import jax.numpy as jnp
import ml_dtypes
import numpy as np
from jax import lax
from jax.experimental import pallas as pl
from jax.experimental.pallas import tpu as pltpu
from jax.sharding import PartitionSpec as P

MESH = pl.DeviceIdType.MESH
BF = jnp.bfloat16
F32 = jnp.float32


def split_np(x):
    hi = x.astype(np.float32).astype(ml_dtypes.bfloat16)
    lo = (x - hi.astype(np.float64)).astype(np.float32).astype(ml_dtypes.bfloat16)
    return hi, lo


def tables(n, radix, rows):
    m = n // radix
    a = np.arange(m)
    blocks = []
    for r in range(radix):
        phase = (a[:, None] * (r + radix * a[None, :])) % n * (2.0 * math.pi / n)
        c, s = np.cos(phase) / math.sqrt(n), np.sin(phase) / math.sqrt(n)
        blocks.append(np.block([[c, s], [-s, c]]))
    b = np.stack(blocks)
    bh, bl = split_np(b)
    row = np.concatenate([bh, bl], axis=1)
    halves = []
    for parity in (0, 1):
        pick = a[(a // rows) % 2 == parity]
        pick = np.concatenate([pick, m + pick])
        halves.append(np.concatenate([bh.transpose(0, 2, 1)[:, :, pick], bl.transpose(0, 2, 1)[:, :, pick]], axis=2))
    col = np.stack(halves, axis=1)
    return row, col


def split(x):
    hi = x.astype(BF)
    return hi, (x - hi.astype(F32)).astype(BF)


def radix4(re, im):
    ar, ai, br, bi = re[0] + re[2], im[0] + im[2], re[0] - re[2], im[0] - im[2]
    cr, ci, dr, di = re[1] + re[3], im[1] + im[3], re[1] - re[3], im[1] - im[3]
    return [(ar + cr, ai + ci), (br - di, bi + dr), (ar - cr, ai - ci), (br + di, bi - dr)]


OWN, Z_IN, Y_IN, ACROSS, ROWS, COLUMNS = range(6)
TUNED = {
    (2, 4, 4, 3, 4): [
        (0, 0, 0), (0, 0, 1), (0, 0, 2), (2, 0, 0, 0), (1, 0, 1, 0), (0, 1, 0), (1, 0, 1, 1), (1, 0, 2, 0),
        (1, 0, 1, 2), (0, 1, 1), (0, 0, 3), (1, 0, 3, 0), (1, 0, 2, 1), (2, 0, 1, 0), (1, 0, 2, 2), (4, 0, 1, 0),
        (1, 1, 1, 0), (1, 0, 3, 1), (0, 1, 2), (2, 0, 3, 0), (1, 0, 3, 2), (4, 0, 2, 0), (4, 0, 0, 0), (4, 0, 3, 0),
        (2, 0, 2, 0), (2, 0, 0, 1), (5, 0, 1, 0, 0), (2, 0, 1, 1), (5, 0, 1, 1, 0), (0, 1, 3), (5, 0, 1, 2, 0), (5, 0, 1, 3, 0),
        (2, 0, 1, 2), (1, 1, 1, 1), (1, 1, 2, 0), (2, 0, 3, 1), (2, 1, 0, 0), (2, 1, 0, 1), (1, 1, 1, 2), (2, 0, 0, 2),
        (4, 1, 1, 0), (5, 0, 0, 0, 0), (3, 1, 0), (4, 0, 1, 1), (4, 0, 0, 1), (1, 1, 2, 1), (2, 0, 2, 1), (2, 0, 2, 2),
        (4, 1, 0, 0), (5, 0, 0, 1, 0), (2, 0, 3, 2), (1, 1, 3, 0), (5, 0, 0, 2, 0), (5, 0, 0, 3, 0), (2, 1, 0, 2), (4, 0, 2, 1),
        (4, 0, 3, 1), (1, 1, 2, 2), (5, 0, 1, 0, 1), (5, 0, 1, 1, 1), (3, 1, 1), (2, 1, 2, 0), (4, 1, 2, 0), (4, 1, 0, 1),
        (5, 0, 1, 2, 1), (2, 1, 1, 0), (5, 0, 1, 3, 1), (5, 0, 0, 0, 1), (3, 1, 2), (2, 1, 2, 1), (1, 1, 3, 1), (5, 0, 0, 1, 1),
        (2, 1, 3, 0), (5, 0, 0, 2, 1), (5, 0, 0, 3, 1), (1, 1, 3, 2), (4, 1, 3, 0), (2, 1, 2, 2), (5, 1, 1, 0, 0), (5, 1, 1, 1, 0),
        (5, 1, 1, 2, 0), (5, 1, 1, 3, 0), (2, 1, 3, 1), (5, 1, 0, 0, 0), (5, 1, 0, 1, 0), (5, 1, 0, 2, 0), (2, 1, 1, 1), (5, 1, 0, 3, 0),
        (2, 1, 1, 2), (4, 1, 1, 1), (2, 1, 3, 2), (4, 1, 2, 1), (4, 1, 3, 1), (5, 1, 1, 0, 1), (5, 1, 1, 1, 1), (5, 1, 1, 2, 1),
        (5, 1, 1, 3, 1), (5, 1, 0, 0, 1), (5, 1, 0, 1, 1), (5, 1, 0, 2, 1), (5, 1, 0, 3, 1),
    ],
}


def program(spc, nz, pieces, parts, radix):
    key = (spc, nz, pieces, len(parts), radix)
    if key in TUNED:
        return TUNED[key]
    order = []
    for l in range(spc):
        order += [(OWN, l, p) for p in range(pieces)]
        end = l == spc - 1
        for j in range(nz):
            order += [(Z_IN, l, j, p) for p in parts if j]
            order += [(Y_IN, l, j, p) for p in parts if not (end and j == 1)]
        order += [(ACROSS, l, p) for p in parts if end]
        order += [(Y_IN, l, 1, p) for p in parts if end]
        order += [(ROWS, l, k, other) for k in range(nz) for other in (0, 1)]
        order += [(COLUMNS, l, tile, rx, phase) for phase in (0, 1) for tile in (1, 0) for rx in range(radix)]
    return order


def kernel(dims, owner_ref, weight_ref, mask_hbm, kern_hbm, rowt_hbm, colt_hbm, out_ref,
           side, held, mask, rowt, colt, lane_perm, stage, field, cols, acc, total, part, blocks,
           loc, k_recv, m_recv, e_recv, z_recv, y_recv, x_recv, p_recv, gone, *kern):
    spc, nk, nz, rows, n, radix = dims
    m = n // radix
    last = spc - 1
    g = lax.axis_index("kgrp")
    t = lax.axis_index("tile")
    x, c = g // 2, g % 2
    z, y = t // 2, t % 2
    xo, co, yo = 1 - x, 1 - c, 1 - y
    x_peer, c_peer = {"kgrp": 2 * xo + c}, {"kgrp": 2 * x + co}
    y_peer = {"tile": 2 * z + yo}

    def at_z(i):
        return {"tile": 2 * i + y}

    unit = 8
    nt = rows // unit
    share = nt // 4
    keep = nt - share
    wide = max(share, 1)
    cuts = [(i, i + wide) for i in range(0, nt, wide)]
    parts = [p for p, cut in enumerate(cuts) if cut[1] <= keep]

    def tiles_of(s, a, b):
        return pl.ds(pl.multiple_of(a * unit + s * (rows - unit * (a + b)), unit), unit * (b - a))

    barrier = pltpu.get_barrier_semaphore()
    for peer in (c_peer, x_peer, y_peer):
        pl.semaphore_signal(barrier, inc=1, device_id=peer, device_id_type=MESH)

    @pl.when(z > 0)
    def _():
        pl.semaphore_signal(barrier, inc=1, device_id=at_z(z - 1), device_id_type=MESH)

    @pl.when(z < nz - 1)
    def _():
        pl.semaphore_signal(barrier, inc=1, device_id=at_z(z + 1), device_id_type=MESH)

    def span(s, p):
        return tiles_of(s, *cuts[p])

    def pieces_of(l, p):
        a, b = cuts[p]
        return [(a, a + 1), (a + 1, b)] if l == p == 0 and b - a > 1 else [(a, b)]

    def candidates(core, p):
        return kern[p].at[pl.ds(core * nk, nk)]

    first_loads = [pltpu.make_async_copy(kern_hbm.at[:, :, span(xo, p)], candidates(c, p), loc.at[3 + p])
                   for p in range(len(cuts))]
    loads = [
        pltpu.make_async_copy(mask_hbm, mask.at[0], loc.at[0]),
        pltpu.make_async_copy(rowt_hbm, rowt, loc.at[1]),
        pltpu.make_async_copy(colt_hbm, colt, loc.at[2]),
    ]
    for load in first_loads + loads:
        load.start()
    for load in first_loads:
        load.wait()
    pl.semaphore_wait(barrier, 3 + jnp.minimum(z, 1) + jnp.minimum(nz - 1 - z, 1))

    groups = {}

    def send(src, dst, recv_sem, device, group, cond=None):
        index, _, size = groups.setdefault(group, (len(groups), cond, 0))
        groups[group] = index, cond, size + math.prod(src.shape) // n
        copy = pltpu.make_async_remote_copy(src_ref=src, dst_ref=dst, send_sem=gone.at[index], recv_sem=recv_sem,
                                            device_id=device, device_id_type=MESH)
        if cond is None:
            copy.start()
        else:
            pl.when(cond)(copy.start)

    def all_gone():
        for index, cond, size in groups.values():
            if size <= n:
                ref = mask.at[0, 0, pl.ds(0, size)]
            elif size <= 2 * n:
                ref = mask.at[0, :, pl.ds(0, size // 2)]
            else:
                ref = mask.at[:, :, pl.ds(0, size // 4)]
            wait = pltpu.make_async_remote_copy(src_ref=ref, dst_ref=ref, send_sem=gone.at[index],
                                                recv_sem=gone.at[index], device_id=c_peer, device_id_type=MESH).wait_send
            if cond is None:
                wait()
            else:
                pl.when(cond)(wait)

    def arrive(ref, recv_sem):
        pltpu.make_async_remote_copy(src_ref=ref, dst_ref=ref, send_sem=recv_sem, recv_sem=recv_sem,
                                     device_id=c_peer, device_id_type=MESH).wait_recv()

    def piece(l, zz, yy, s, p):
        return held.at[l, zz, yy, :, span(s, p)]

    for p in range(len(cuts)):
        src = candidates(c, p)
        send(src, src, k_recv.at[p], c_peer, "core")
    send(mask_hbm, mask.at[1], m_recv.at[0], c_peer, "mask")

    owners = [owner_ref[c * spc + l] for l in range(spc)]
    for p in range(len(cuts)):
        arrive(candidates(co, p), k_recv.at[p])
        for l in range(spc):
            side[x, l, :, span(xo, p)] = kern[p][owners[l] % (2 * nk)]
        for i, sub in enumerate(pieces_of(0, p)):
            src = side.at[x, 0, :, tiles_of(xo, *sub)]
            send(src, src, e_recv.at[0, p + (len(cuts) if i else 0)], x_peer, "core")
    for l in range(1, spc):
        for p in range(len(cuts)):
            src = side.at[x, l, :, span(xo, p)]
            send(src, src, e_recv.at[l, p], x_peer, "core")

    half = n // 2
    wide_lane = m // 2
    src_lane = lax.broadcasted_iota(jnp.int32, (half, half), 0)
    dst_lane = lax.broadcasted_iota(jnp.int32, (half, half), 1)
    perm = jnp.where((src_lane % wide_lane) * radix + src_lane // wide_lane == dst_lane, 1.0, 0.0).astype(BF)
    lane_perm[:half] = perm
    lane_perm[half:] = perm

    def own(l, p):
        mine = owners[l] // (2 * nk) == x
        for i, sub in enumerate(pieces_of(l, p)):
            at = tiles_of(x, *sub)
            arrive(side.at[xo, l, :, at], e_recv.at[l, p + (len(cuts) if i else 0)])
            held[l, z, y, :, at] = jnp.where(mine, side[x, l, :, at], side[xo, l, :, at])
            if p in parts:
                here = held.at[l, z, y, :, at]
                send(here, here, y_recv.at[l, z, p], y_peer, "core")
                send(here, here, z_recv.at[l, z, p], at_z(z - 1), "down", z > 0)
                send(here, here, z_recv.at[l, z, p], at_z(z + 1), "up", z < nz - 1)

    def across(l, p):
        here = piece(l, z, yo, x, p)
        send(here, here, y_recv.at[l, z, p], at_z(z - 1), "down", z > 0)
        send(here, here, y_recv.at[l, z, p], at_z(z + 1), "up", z < nz - 1)

    def share_x(l, zz, yy, group, cond=None):
        if share:
            here = piece(l, zz, yy, x, 0)
            send(here, here, x_recv.at[l, zz, yy], x_peer, group, cond)

    def z_in(l, j, p):
        for s, zz, have, dest, more in ((1, z + j, z + j < nz, z - 1, z > 0), (-1, z - j, z >= j, z + 1, z < nz - 1)):
            here = piece(l, zz, y, x, p)
            pl.when(have)(functools.partial(arrive, here, z_recv.at[l, zz, p]))
            if j < nz - 1:
                send(here, here, z_recv.at[l, zz, p], at_z(dest), ("relay", s * j), have & more)
            if l != last or j > 1:
                send(here, here, y_recv.at[l, zz, p], y_peer, ("on", s * j), have)
            if p == 0:
                share_x(l, zz, y, ("on", s * j), have)

    def y_in(l, j, p):
        if j == 0:
            arrive(piece(l, z, yo, x, p), y_recv.at[l, z, p])
            if p == 0:
                share_x(l, z, yo, "core")
            return
        for s, zz, have in ((1, z + j, z + j < nz), (-1, z - j, z >= j)):
            pl.when(have)(functools.partial(arrive, piece(l, zz, yo, x, p), y_recv.at[l, zz, p]))
            if p == 0:
                share_x(l, zz, yo, ("on", s * j), have)

    def near(k):
        if k == 0:
            return z
        low = jnp.minimum(z, nz - 1 - z)
        both = z + (k + 1) // 2 if k % 2 else z - k // 2
        one = jnp.where(low == z, z + k - low, z - k + low)
        return jnp.where(k <= 2 * low, both, one)

    def x_in(l, k, yy):
        if share and not (k == 0 and yy is y):
            arrive(piece(l, near(k), yy, xo, 0), x_recv.at[l, near(k), yy])

    strip = 16
    waiting = []

    def product(l, k, yy, slot, tile, strip_index):
        zi = near(k)
        lo_row = strip * strip_index
        at = pl.ds(pl.multiple_of((2 * zi + yy) * rows + lo_row, strip), strip)
        src = slice(lo_row, lo_row + strip)
        to = slice(tile * rows + lo_row, tile * rows + lo_row + strip)
        re, im = [], []
        for q in range(radix):
            lanes = slice(q * m, (q + 1) * m)
            kr, ki = held[l, zi, yy, 0, src, lanes], held[l, zi, yy, 1, src, lanes]
            mr, mi = mask[tile, 0, at, lanes], mask[tile, 1, at, lanes]
            re.append(mr * kr - mi * ki)
            im.append(mr * ki + mi * kr)
        for r, pair in enumerate(radix4(re, im)):
            for p, v in enumerate(pair):
                hi, lo = split(v)
                stage[slot, r, to, p * m:(p + 1) * m] = hi
                stage[slot, r, to, (2 + p) * m:(3 + p) * m] = lo

    def row_matmul(l, k, yy, slot, r):
        hi, lo = stage[slot, r, :, :2 * m], stage[slot, r, :, 2 * m:]
        th, tl = rowt[r, :2 * m], rowt[r, 2 * m:]
        done = jnp.dot(jnp.concatenate([hi, lo, hi], 1), jnp.concatenate([th, th, tl], 0),
                       preferred_element_type=F32)
        at = pl.ds(pl.multiple_of((2 * near(k) + yy) * rows, rows), rows)
        for tile in range(2):
            field[l, r, tile, at] = done[tile * rows:(tile + 1) * rows]

    def woven(first, second):
        count = max(len(first), len(second))
        for i in range(count):
            for group in (first, second):
                for work in group[i * len(group) // count:(i + 1) * len(group) // count]:
                    work()

    def held_matmuls():
        works = [functools.partial(row_matmul, *waiting[0], r) for r in range(radix)] if waiting else []
        waiting.clear()
        return works

    def row_step(l, k, other):
        yy = yo if other else y
        x_in(l, k, yy)
        slot = 1 - waiting[0][3] if waiting else 0
        products = [functools.partial(product, l, k, yy, slot, tile, i)
                    for i in range(rows // strip) for tile in range(2)]
        woven(held_matmuls(), products)
        waiting.append((l, k, yy, slot))

    def middle(l, tile, ry, phase):
        own_half = y if phase == 0 else yo

        def strip_of(i):
            at = strip * i
            base = at // rows * 2 * rows + at % rows
            lanes = slice(ry * m, (ry + 1) * m)
            from_rows = [pl.ds(pl.multiple_of(k * m + base + own_half * rows, strip), strip) for k in range(radix)]
            re = [field[l, ry, tile, rows_at, :m] for rows_at in from_rows]
            im = [field[l, ry, tile, rows_at, m:] for rows_at in from_rows]
            for rx, pair in enumerate(radix4(re, im)):
                for p, v in enumerate(pair):
                    hi, lo = split(v)
                    to = p * (m // 2) + at
                    cols[tile, rx, to:to + strip, lanes] = hi
                    cols[tile, rx, m + to:m + to + strip, lanes] = lo
        return [functools.partial(strip_of, i) for i in range(m // 2 // strip)]

    def columns(l, tile, rx, phase):
        hi, lo = cols[tile, rx, :m], cols[tile, rx, m:]
        own_half = y if phase == 0 else yo
        th, tl = colt[rx, own_half, :, :m], colt[rx, own_half, :, m:]
        done = (jnp.dot(jnp.concatenate([th, tl], 1), jnp.concatenate([hi, hi], 0), preferred_element_type=F32)
                + jnp.dot(th, lo, preferred_element_type=F32))
        if phase == 0:
            acc[tile, rx] = done
            return
        done += acc[tile, rx]
        power = (done[:m] * done[:m] + done[m:] * done[m:]) * weight_ref[c * spc + l]
        if l == 0:
            total[tile, rx] = power
        else:
            total[tile, rx] += power

    def column_step(l, tile, rx, phase):
        if rx == 0 and waiting and waiting[0][0] == l:
            woven(held_matmuls(), [])
        if rx == 0 and tile == 1:
            for ry in range(radix):
                woven(middle(l, tile, ry, phase), [])
        woven([functools.partial(columns, l, tile, rx, phase)], middle(l, 0, rx, phase) if tile == 1 else [])
        if l == last and tile == 1 and phase == 1:
            for done in [rx - 1] if rx < radix - 1 else [rx - 1, rx]:
                if done >= 0:
                    send(total.at[1, done], part.at[done], p_recv.at[0], c_peer, "part")

    steps = (own, z_in, y_in, across, row_step, column_step)
    first_row = True
    for op, *args in program(spc, nz, len(cuts), parts, radix):
        if op == 4 and first_row:
            first_row = False
            for load in loads:
                load.wait()
            arrive(mask.at[1], m_recv.at[0])
        steps[op](*args)

    arrive(part, p_recv.at[0])
    low = lax.broadcasted_iota(jnp.int32, (m, m), 1) < wide_lane
    perm = lane_perm[...]
    for rx in range(radix):
        lanes = [total[0, rx, :, r * m:(r + 1) * m] + part[rx, :, r * m:(r + 1) * m] for r in range(radix)]
        turned = [pltpu.roll(v, wide_lane, 1) for v in lanes]
        for h in range(2):
            pairs = [jnp.where(low, *((lanes[r], turned[r + 1]) if h == 0 else (turned[r], lanes[r + 1])))
                     for r in range(0, radix, 2)]
            hi, lo = split(jnp.concatenate(pairs, 1))
            image = jnp.dot(jnp.concatenate([hi, lo], 1), perm, preferred_element_type=F32)
            for q in range(radix // 2):
                blocks[h * (radix // 2) + q, pl.ds(rx, m, stride=radix), :] = image[:, q * m:(q + 1) * m]
    for q in range(radix):
        out_ref[:, q * m:(q + 1) * m] = blocks[q]
    all_gone()


def local(mesh_shape, mask_spectrum, kernels, owner_table, step_weight):
    groups, tiles = mesh_shape
    nk, _, rows, n = kernels.shape
    steps = owner_table.shape[0]
    radix = 4
    m = n // radix
    spc = steps // 2
    nz = tiles // 2
    most = min(rows // 8, 4)
    kept = most - (rows // 8 >= 4)
    rowt, colt = tables(n, radix, rows)
    dma = pltpu.SemaphoreType.DMA
    any_spec = pl.BlockSpec(memory_space=pl.ANY)
    smem = pl.BlockSpec(memory_space=pltpu.SMEM)
    out = pl.pallas_call(
        functools.partial(kernel, (spc, nk, nz, rows, n, radix)),
        out_shape=pltpu.VMEM((n, n), F32),
        in_specs=[smem, smem, any_spec, any_spec, any_spec, any_spec],
        out_specs=pl.BlockSpec(memory_space=pltpu.VMEM),
        scratch_shapes=[
            pltpu.VMEM((2, spc, 2, rows, n), F32),
            pltpu.VMEM((spc, nz, 2, 2, rows, n), F32),
            pltpu.VMEM((2, 2, n, n), F32),
            pltpu.VMEM(rowt.shape, BF),
            pltpu.VMEM(colt.shape, BF),
            pltpu.VMEM((n, n // 2), BF),
            pltpu.VMEM((2, radix, 2 * rows, 4 * m), BF),
            pltpu.VMEM((spc, radix, 2, n, 2 * m), F32),
            pltpu.VMEM((2, radix, 2 * m, n), BF),
            pltpu.VMEM((2, radix, 2 * m, n), F32),
            pltpu.VMEM((2, radix, m, n), F32),
            pltpu.VMEM((radix, m, n), F32),
            pltpu.VMEM((radix, n, m), F32),
            dma((3 + most,)), dma((most,)), dma((1,)), dma((spc, most + 1)), dma((spc, nz, kept)), dma((spc, nz, kept)),
            dma((spc, nz, 2)), dma((1,)), dma((4 * nz + 2,)),
        ] + [pltpu.VMEM((2 * nk, 2, rows // most, n), F32)] * most,
        compiler_params=pltpu.CompilerParams(collective_id=0, has_side_effects=True, vmem_limit_bytes=54 * 1024 * 1024),
    )(owner_table, step_weight, mask_spectrum[0], kernels, jnp.asarray(rowt), jnp.asarray(colt))
    return out[None]


def solution(mesh):
    in_specs = (P(("kgrp", "tile"), None, None, None), P("kgrp", None, "tile", None), P(), P())
    out_specs = P(("kgrp", "tile"), None, None)
    body = functools.partial(local, (mesh.shape["kgrp"], mesh.shape["tile"]))
    return jax.shard_map(body, mesh=mesh, in_specs=in_specs, out_specs=out_specs, check_vma=False)
```

```python
import functools
import math

import jax
import jax.numpy as jnp
import ml_dtypes
import numpy as np
from jax import lax
from jax.experimental import pallas as pl
from jax.experimental.pallas import tpu as pltpu
from jax.sharding import PartitionSpec as P

MESH = pl.DeviceIdType.MESH
BF = jnp.bfloat16
F32 = jnp.float32


def split_np(x):
    hi = x.astype(np.float32).astype(ml_dtypes.bfloat16)
    lo = (x - hi.astype(np.float64)).astype(np.float32).astype(ml_dtypes.bfloat16)
    return hi, lo


def tables(n, radix, rows):
    m = n // radix
    a = np.arange(m)
    blocks = []
    for r in range(radix):
        phase = (a[:, None] * (r + radix * a[None, :])) % n * (2.0 * math.pi / n)
        c, s = np.cos(phase) / math.sqrt(n), np.sin(phase) / math.sqrt(n)
        blocks.append(np.block([[c, s], [-s, c]]))
    b = np.stack(blocks)
    bh, bl = split_np(b)
    row = np.concatenate([bh, bl], axis=1)
    halves = []
    for parity in (0, 1):
        pick = a[(a // rows) % 2 == parity]
        pick = np.concatenate([pick, m + pick])
        halves.append(np.concatenate([bh.transpose(0, 2, 1)[:, :, pick], bl.transpose(0, 2, 1)[:, :, pick]], axis=2))
    col = np.stack(halves, axis=1)
    return row, col


def split(x):
    hi = x.astype(BF)
    return hi, (x - hi.astype(F32)).astype(BF)


def radix4(re, im):
    ar, ai, br, bi = re[0] + re[2], im[0] + im[2], re[0] - re[2], im[0] - im[2]
    cr, ci, dr, di = re[1] + re[3], im[1] + im[3], re[1] - re[3], im[1] - im[3]
    return [(ar + cr, ai + ci), (br - di, bi + dr), (ar - cr, ai - ci), (br + di, bi - dr)]


OWN, Z_IN, Y_IN, ACROSS, ROWS, COLUMNS = range(6)
TUNED = {
    (2, 4, 4, 3, 4): [
        (0, 0, 0), (0, 0, 1), (0, 0, 2), (1, 0, 1, 0), (1, 0, 1, 1), (0, 1, 0), (1, 0, 2, 0), (1, 0, 1, 2),
        (0, 0, 3), (1, 0, 2, 1), (2, 0, 1, 0), (1, 0, 3, 0), (1, 0, 2, 2), (2, 0, 0, 0), (2, 0, 0, 1), (0, 1, 1),
        (4, 0, 2, 0), (1, 0, 3, 1), (2, 0, 0, 2), (1, 1, 1, 0), (0, 1, 2), (2, 0, 3, 0), (2, 0, 1, 1), (2, 0, 2, 0),
        (2, 1, 0, 0), (1, 0, 3, 2), (4, 0, 3, 0), (4, 0, 1, 0), (4, 0, 0, 0), (1, 1, 2, 0), (1, 1, 1, 1), (2, 0, 1, 2),
        (5, 0, 1, 0, 0), (4, 0, 0, 1), (5, 0, 1, 1, 0), (5, 0, 1, 2, 0), (5, 0, 1, 3, 0), (1, 1, 1, 2), (2, 0, 2, 1), (3, 1, 0),
        (5, 0, 0, 0, 0), (2, 0, 3, 1), (4, 1, 1, 0), (2, 0, 2, 2), (1, 1, 3, 0), (4, 0, 2, 1), (5, 0, 0, 1, 0), (4, 0, 1, 1),
        (2, 0, 3, 2), (1, 1, 2, 1), (2, 1, 0, 1), (5, 0, 0, 2, 0), (5, 0, 0, 3, 0), (4, 0, 3, 1), (5, 0, 1, 0, 1), (1, 1, 2, 2),
        (3, 1, 1), (5, 0, 1, 1, 1), (2, 1, 0, 2), (5, 0, 1, 2, 1), (3, 1, 2), (4, 1, 0, 1), (0, 1, 3), (2, 1, 1, 0),
        (2, 1, 2, 0), (5, 0, 1, 3, 1), (4, 1, 2, 0), (5, 0, 0, 0, 1), (2, 1, 2, 1), (1, 1, 3, 1), (5, 0, 0, 1, 1), (5, 0, 0, 2, 1),
        (5, 0, 0, 3, 1), (2, 1, 3, 0), (4, 1, 0, 0), (1, 1, 3, 2), (4, 1, 3, 0), (5, 1, 1, 0, 0), (5, 1, 1, 1, 0), (5, 1, 1, 2, 0),
        (5, 1, 1, 3, 0), (2, 1, 2, 2), (5, 1, 0, 0, 0), (2, 1, 1, 1), (5, 1, 0, 1, 0), (5, 1, 0, 2, 0), (5, 1, 0, 3, 0), (2, 1, 1, 2),
        (4, 1, 1, 1), (4, 1, 2, 1), (2, 1, 3, 1), (2, 1, 3, 2), (4, 1, 3, 1), (5, 1, 1, 0, 1), (5, 1, 1, 1, 1), (5, 1, 1, 2, 1),
        (5, 1, 1, 3, 1), (5, 1, 0, 0, 1), (5, 1, 0, 1, 1), (5, 1, 0, 2, 1), (5, 1, 0, 3, 1),
    ],
}


def program(spc, nz, pieces, parts, radix):
    key = (spc, nz, pieces, len(parts), radix)
    if key in TUNED:
        return TUNED[key]
    order = []
    for l in range(spc):
        order += [(OWN, l, p) for p in range(pieces)]
        end = l == spc - 1
        for j in range(nz):
            order += [(Z_IN, l, j, p) for p in parts if j]
            order += [(Y_IN, l, j, p) for p in parts if not (end and j == 1)]
        order += [(ACROSS, l, p) for p in parts if end]
        order += [(Y_IN, l, 1, p) for p in parts if end]
        order += [(ROWS, l, k, other) for k in range(nz) for other in (0, 1)]
        order += [(COLUMNS, l, tile, rx, phase) for phase in (0, 1) for tile in (1, 0) for rx in range(radix)]
    return order


def kernel(dims, owner_ref, weight_ref, mask_hbm, kern_hbm, rowt_hbm, colt_hbm, out_ref,
           side, held, mask, rowt, colt, lane_perm, stage, field, cols, acc, total, part, blocks,
           loc, k_recv, m_recv, e_recv, z_recv, y_recv, x_recv, p_recv, gone, *kern):
    spc, nk, nz, rows, n, radix = dims
    m = n // radix
    last = spc - 1
    g = lax.axis_index("kgrp")
    t = lax.axis_index("tile")
    x, c = g // 2, g % 2
    z, y = t // 2, t % 2
    xo, co, yo = 1 - x, 1 - c, 1 - y
    x_peer, c_peer = {"kgrp": 2 * xo + c}, {"kgrp": 2 * x + co}
    y_peer = {"tile": 2 * z + yo}

    def at_z(i):
        return {"tile": 2 * i + y}

    unit = 8
    nt = rows // unit
    share = nt // 4
    keep = nt - share
    wide = max(share, 1)
    cuts = [(i, i + wide) for i in range(0, nt, wide)]
    parts = [p for p, cut in enumerate(cuts) if cut[1] <= keep]

    def tiles_of(s, a, b):
        return pl.ds(pl.multiple_of(a * unit + s * (rows - unit * (a + b)), unit), unit * (b - a))

    barrier = pltpu.get_barrier_semaphore()
    for peer in (c_peer, x_peer, y_peer):
        pl.semaphore_signal(barrier, inc=1, device_id=peer, device_id_type=MESH)

    @pl.when(z > 0)
    def _():
        pl.semaphore_signal(barrier, inc=1, device_id=at_z(z - 1), device_id_type=MESH)

    @pl.when(z < nz - 1)
    def _():
        pl.semaphore_signal(barrier, inc=1, device_id=at_z(z + 1), device_id_type=MESH)

    def span(s, p):
        return tiles_of(s, *cuts[p])

    def pieces_of(l, p):
        a, b = cuts[p]
        return [(a, a + 1), (a + 1, b)] if l == p == 0 and b - a > 1 else [(a, b)]

    def candidates(core, p):
        return kern[p].at[pl.ds(core * nk, nk)]

    first_loads = [pltpu.make_async_copy(kern_hbm.at[:, :, span(xo, p)], candidates(c, p), loc.at[3 + p])
                   for p in range(len(cuts))]
    loads = [
        pltpu.make_async_copy(mask_hbm, mask.at[0], loc.at[0]),
        pltpu.make_async_copy(rowt_hbm, rowt, loc.at[1]),
        pltpu.make_async_copy(colt_hbm, colt, loc.at[2]),
    ]
    for load in first_loads + loads:
        load.start()
    for load in first_loads:
        load.wait()
    pl.semaphore_wait(barrier, 3 + jnp.minimum(z, 1) + jnp.minimum(nz - 1 - z, 1))

    groups = {}

    def send(src, dst, recv_sem, device, group, cond=None):
        index, _, size = groups.setdefault(group, (len(groups), cond, 0))
        groups[group] = index, cond, size + math.prod(src.shape) // n
        copy = pltpu.make_async_remote_copy(src_ref=src, dst_ref=dst, send_sem=gone.at[index], recv_sem=recv_sem,
                                            device_id=device, device_id_type=MESH)
        if cond is None:
            copy.start()
        else:
            pl.when(cond)(copy.start)

    def all_gone():
        for index, cond, size in groups.values():
            if size <= n:
                ref = mask.at[0, 0, pl.ds(0, size)]
            elif size <= 2 * n:
                ref = mask.at[0, :, pl.ds(0, size // 2)]
            else:
                ref = mask.at[:, :, pl.ds(0, size // 4)]
            wait = pltpu.make_async_remote_copy(src_ref=ref, dst_ref=ref, send_sem=gone.at[index],
                                                recv_sem=gone.at[index], device_id=c_peer, device_id_type=MESH).wait_send
            if cond is None:
                wait()
            else:
                pl.when(cond)(wait)

    def arrive(ref, recv_sem):
        pltpu.make_async_remote_copy(src_ref=ref, dst_ref=ref, send_sem=recv_sem, recv_sem=recv_sem,
                                     device_id=c_peer, device_id_type=MESH).wait_recv()

    def piece(l, zz, yy, s, p):
        return held.at[l, zz, yy, :, span(s, p)]

    for p in range(len(cuts)):
        src = candidates(c, p)
        send(src, src, k_recv.at[p], c_peer, "core")
    owners = [owner_ref[c * spc + l] for l in range(spc)]
    for p in range(len(cuts)):
        arrive(candidates(co, p), k_recv.at[p])
        for l in range(spc):
            side[x, l, :, span(xo, p)] = kern[p][owners[l] % (2 * nk)]
        for i, sub in enumerate(pieces_of(0, p)):
            src = side.at[x, 0, :, tiles_of(xo, *sub)]
            send(src, src, e_recv.at[0, p + (len(cuts) if i else 0)], x_peer, "core")
    for l in range(1, spc):
        for p in range(len(cuts)):
            src = side.at[x, l, :, span(xo, p)]
            send(src, src, e_recv.at[l, p], x_peer, "core")

    half = n // 2
    wide_lane = m // 2
    src_lane = lax.broadcasted_iota(jnp.int32, (half, half), 0)
    dst_lane = lax.broadcasted_iota(jnp.int32, (half, half), 1)
    perm = jnp.where((src_lane % wide_lane) * radix + src_lane // wide_lane == dst_lane, 1.0, 0.0).astype(BF)
    lane_perm[:half] = perm
    lane_perm[half:] = perm

    def own(l, p):
        mine = owners[l] // (2 * nk) == x
        for i, sub in enumerate(pieces_of(l, p)):
            at = tiles_of(x, *sub)
            arrive(side.at[xo, l, :, at], e_recv.at[l, p + (len(cuts) if i else 0)])
            held[l, z, y, :, at] = jnp.where(mine, side[x, l, :, at], side[xo, l, :, at])
            if p in parts:
                here = held.at[l, z, y, :, at]
                send(here, here, y_recv.at[l, z, p], y_peer, "core")
                send(here, here, z_recv.at[l, z, p], at_z(z - 1), "down", z > 0)
                send(here, here, z_recv.at[l, z, p], at_z(z + 1), "up", z < nz - 1)

    def across(l, p):
        here = piece(l, z, yo, x, p)
        send(here, here, y_recv.at[l, z, p], at_z(z - 1), "down", z > 0)
        send(here, here, y_recv.at[l, z, p], at_z(z + 1), "up", z < nz - 1)

    def share_x(l, zz, yy, group, cond=None):
        if share:
            here = piece(l, zz, yy, x, 0)
            send(here, here, x_recv.at[l, zz, yy], x_peer, group, cond)

    def z_in(l, j, p):
        for s, zz, have, dest, more in ((1, z + j, z + j < nz, z - 1, z > 0), (-1, z - j, z >= j, z + 1, z < nz - 1)):
            here = piece(l, zz, y, x, p)
            pl.when(have)(functools.partial(arrive, here, z_recv.at[l, zz, p]))
            if j < nz - 1:
                send(here, here, z_recv.at[l, zz, p], at_z(dest), ("relay", s * j), have & more)
            if l != last or j > 1:
                send(here, here, y_recv.at[l, zz, p], y_peer, ("on", s * j), have)
            if p == 0:
                share_x(l, zz, y, ("on", s * j), have)

    def y_in(l, j, p):
        if j == 0:
            arrive(piece(l, z, yo, x, p), y_recv.at[l, z, p])
            if p == 0:
                share_x(l, z, yo, "core")
            return
        for s, zz, have in ((1, z + j, z + j < nz), (-1, z - j, z >= j)):
            pl.when(have)(functools.partial(arrive, piece(l, zz, yo, x, p), y_recv.at[l, zz, p]))
            if p == 0:
                share_x(l, zz, yo, ("on", s * j), have)

    def near(k):
        if k == 0:
            return z
        low = jnp.minimum(z, nz - 1 - z)
        both = z + (k + 1) // 2 if k % 2 else z - k // 2
        one = jnp.where(low == z, z + k - low, z - k + low)
        return jnp.where(k <= 2 * low, both, one)

    def x_in(l, k, yy):
        if share and not (k == 0 and yy is y):
            arrive(piece(l, near(k), yy, xo, 0), x_recv.at[l, near(k), yy])

    strip = 16
    waiting = []

    def product(l, k, yy, slot, tile, strip_index):
        zi = near(k)
        lo_row = strip * strip_index
        at = pl.ds(pl.multiple_of((2 * zi + yy) * rows + lo_row, strip), strip)
        src = slice(lo_row, lo_row + strip)
        to = slice(tile * rows + lo_row, tile * rows + lo_row + strip)
        re, im = [], []
        for q in range(radix):
            lanes = slice(q * m, (q + 1) * m)
            kr, ki = held[l, zi, yy, 0, src, lanes], held[l, zi, yy, 1, src, lanes]
            mr, mi = mask[tile, 0, at, lanes], mask[tile, 1, at, lanes]
            re.append(mr * kr - mi * ki)
            im.append(mr * ki + mi * kr)
        for r, pair in enumerate(radix4(re, im)):
            for p, v in enumerate(pair):
                hi, lo = split(v)
                stage[slot, r, to, p * m:(p + 1) * m] = hi
                stage[slot, r, to, (2 + p) * m:(3 + p) * m] = lo

    def row_matmul(l, k, yy, slot, r):
        hi, lo = stage[slot, r, :, :2 * m], stage[slot, r, :, 2 * m:]
        th, tl = rowt[r, :2 * m], rowt[r, 2 * m:]
        done = jnp.dot(jnp.concatenate([hi, lo, hi], 1), jnp.concatenate([th, th, tl], 0),
                       preferred_element_type=F32)
        at = pl.ds(pl.multiple_of((2 * near(k) + yy) * rows, rows), rows)
        for tile in range(2):
            field[l, r, tile, at] = done[tile * rows:(tile + 1) * rows]

    def woven(first, second):
        count = max(len(first), len(second))
        for i in range(count):
            for group in (first, second):
                for work in group[i * len(group) // count:(i + 1) * len(group) // count]:
                    work()

    def held_matmuls():
        works = [functools.partial(row_matmul, *waiting[0], r) for r in range(radix)] if waiting else []
        waiting.clear()
        return works

    def row_step(l, k, other):
        yy = yo if other else y
        x_in(l, k, yy)
        slot = 1 - waiting[0][3] if waiting else 0
        products = [functools.partial(product, l, k, yy, slot, tile, i)
                    for i in range(rows // strip) for tile in range(2)]
        woven(held_matmuls(), products)
        waiting.append((l, k, yy, slot))

    def middle(l, tile, ry, phase):
        own_half = y if phase == 0 else yo

        def strip_of(i):
            at = strip * i
            base = at // rows * 2 * rows + at % rows
            lanes = slice(ry * m, (ry + 1) * m)
            from_rows = [pl.ds(pl.multiple_of(k * m + base + own_half * rows, strip), strip) for k in range(radix)]
            re = [field[l, ry, tile, rows_at, :m] for rows_at in from_rows]
            im = [field[l, ry, tile, rows_at, m:] for rows_at in from_rows]
            for rx, pair in enumerate(radix4(re, im)):
                for p, v in enumerate(pair):
                    hi, lo = split(v)
                    to = p * (m // 2) + at
                    cols[tile, rx, to:to + strip, lanes] = hi
                    cols[tile, rx, m + to:m + to + strip, lanes] = lo
        return [functools.partial(strip_of, i) for i in range(m // 2 // strip)]

    def columns(l, tile, rx, phase):
        hi, lo = cols[tile, rx, :m], cols[tile, rx, m:]
        own_half = y if phase == 0 else yo
        th, tl = colt[rx, own_half, :, :m], colt[rx, own_half, :, m:]
        done = (jnp.dot(jnp.concatenate([th, tl], 1), jnp.concatenate([hi, hi], 0), preferred_element_type=F32)
                + jnp.dot(th, lo, preferred_element_type=F32))
        if phase == 0:
            acc[tile, rx] = done
            return
        done += acc[tile, rx]
        power = (done[:m] * done[:m] + done[m:] * done[m:]) * weight_ref[c * spc + l]
        if l == 0:
            total[tile, rx] = power
        else:
            total[tile, rx] += power

    def column_step(l, tile, rx, phase):
        if rx == 0 and waiting and waiting[0][0] == l:
            woven(held_matmuls(), [])
        if rx == 0 and tile == 1:
            for ry in range(radix):
                woven(middle(l, tile, ry, phase), [])
        woven([functools.partial(columns, l, tile, rx, phase)], middle(l, 0, rx, phase) if tile == 1 else [])
        if l == last and tile == 1 and phase == 1:
            for done in [rx - 1] if rx < radix - 1 else [rx - 1, rx]:
                if done >= 0:
                    send(total.at[1, done], part.at[done], p_recv.at[0], c_peer, "part")

    steps = (own, z_in, y_in, across, row_step, column_step)
    first_row = mask_unsent = True
    for op, *args in program(spc, nz, len(cuts), parts, radix):
        if op == 4 and first_row:
            first_row = False
            for load in loads:
                load.wait()
            arrive(mask.at[1], m_recv.at[0])
        steps[op](*args)
        if mask_unsent and (op, *args) == (OWN, 0, min(1, len(cuts) - 1)):
            mask_unsent = False
            send(mask_hbm, mask.at[1], m_recv.at[0], c_peer, "mask")

    arrive(part, p_recv.at[0])
    low = lax.broadcasted_iota(jnp.int32, (m, m), 1) < wide_lane
    perm = lane_perm[...]
    for rx in range(radix):
        lanes = [total[0, rx, :, r * m:(r + 1) * m] + part[rx, :, r * m:(r + 1) * m] for r in range(radix)]
        turned = [pltpu.roll(v, wide_lane, 1) for v in lanes]
        for h in range(2):
            pairs = [jnp.where(low, *((lanes[r], turned[r + 1]) if h == 0 else (turned[r], lanes[r + 1])))
                     for r in range(0, radix, 2)]
            hi, lo = split(jnp.concatenate(pairs, 1))
            image = jnp.dot(jnp.concatenate([hi, lo], 1), perm, preferred_element_type=F32)
            for q in range(radix // 2):
                blocks[h * (radix // 2) + q, pl.ds(rx, m, stride=radix), :] = image[:, q * m:(q + 1) * m]
    for q in range(radix):
        out_ref[:, q * m:(q + 1) * m] = blocks[q]
    all_gone()


def local(mesh_shape, mask_spectrum, kernels, owner_table, step_weight):
    groups, tiles = mesh_shape
    nk, _, rows, n = kernels.shape
    steps = owner_table.shape[0]
    radix = 4
    m = n // radix
    spc = steps // 2
    nz = tiles // 2
    most = min(rows // 8, 4)
    kept = most - (rows // 8 >= 4)
    rowt, colt = tables(n, radix, rows)
    dma = pltpu.SemaphoreType.DMA
    any_spec = pl.BlockSpec(memory_space=pl.ANY)
    smem = pl.BlockSpec(memory_space=pltpu.SMEM)
    out = pl.pallas_call(
        functools.partial(kernel, (spc, nk, nz, rows, n, radix)),
        out_shape=pltpu.VMEM((n, n), F32),
        in_specs=[smem, smem, any_spec, any_spec, any_spec, any_spec],
        out_specs=pl.BlockSpec(memory_space=pltpu.VMEM),
        scratch_shapes=[
            pltpu.VMEM((2, spc, 2, rows, n), F32),
            pltpu.VMEM((spc, nz, 2, 2, rows, n), F32),
            pltpu.VMEM((2, 2, n, n), F32),
            pltpu.VMEM(rowt.shape, BF),
            pltpu.VMEM(colt.shape, BF),
            pltpu.VMEM((n, n // 2), BF),
            pltpu.VMEM((2, radix, 2 * rows, 4 * m), BF),
            pltpu.VMEM((spc, radix, 2, n, 2 * m), F32),
            pltpu.VMEM((2, radix, 2 * m, n), BF),
            pltpu.VMEM((2, radix, 2 * m, n), F32),
            pltpu.VMEM((2, radix, m, n), F32),
            pltpu.VMEM((radix, m, n), F32),
            pltpu.VMEM((radix, n, m), F32),
            dma((3 + most,)), dma((most,)), dma((1,)), dma((spc, most + 1)), dma((spc, nz, kept)), dma((spc, nz, kept)),
            dma((spc, nz, 2)), dma((1,)), dma((4 * nz + 2,)),
        ] + [pltpu.VMEM((2 * nk, 2, rows // most, n), F32)] * most,
        compiler_params=pltpu.CompilerParams(collective_id=0, has_side_effects=True, vmem_limit_bytes=54 * 1024 * 1024),
    )(owner_table, step_weight, mask_spectrum[0], kernels, jnp.asarray(rowt), jnp.asarray(colt))
    return out[None]


def solution(mesh):
    in_specs = (P(("kgrp", "tile"), None, None, None), P("kgrp", None, "tile", None), P(), P())
    out_specs = P(("kgrp", "tile"), None, None)
    body = functools.partial(local, (mesh.shape["kgrp"], mesh.shape["tile"]))
    return jax.shard_map(body, mesh=mesh, in_specs=in_specs, out_specs=out_specs, check_vma=False)
```

```python
import functools
import math

import jax
import jax.numpy as jnp
import ml_dtypes
import numpy as np
from jax import lax
from jax.experimental import pallas as pl
from jax.experimental.pallas import tpu as pltpu
from jax.sharding import PartitionSpec as P

MESH = pl.DeviceIdType.MESH
BF = jnp.bfloat16
F32 = jnp.float32


def split_np(x):
    hi = x.astype(np.float32).astype(ml_dtypes.bfloat16)
    lo = (x - hi.astype(np.float64)).astype(np.float32).astype(ml_dtypes.bfloat16)
    return hi, lo


def tables(n, radix, rows):
    m = n // radix
    a = np.arange(m)
    blocks = []
    for r in range(radix):
        phase = (a[:, None] * (r + radix * a[None, :])) % n * (2.0 * math.pi / n)
        c, s = np.cos(phase) / math.sqrt(n), np.sin(phase) / math.sqrt(n)
        blocks.append(np.block([[c, s], [-s, c]]))
    b = np.stack(blocks)
    bh, bl = split_np(b)
    row = np.concatenate([bh, bl], axis=1)
    halves = []
    for parity in (0, 1):
        pick = a[(a // rows) % 2 == parity]
        pick = np.concatenate([pick, m + pick])
        halves.append(np.concatenate([bh.transpose(0, 2, 1)[:, :, pick], bl.transpose(0, 2, 1)[:, :, pick]], axis=2))
    col = np.stack(halves, axis=1)
    return row, col


def split(x):
    hi = x.astype(BF)
    return hi, (x - hi.astype(F32)).astype(BF)


def radix4(re, im):
    ar, ai, br, bi = re[0] + re[2], im[0] + im[2], re[0] - re[2], im[0] - im[2]
    cr, ci, dr, di = re[1] + re[3], im[1] + im[3], re[1] - re[3], im[1] - im[3]
    return [(ar + cr, ai + ci), (br - di, bi + dr), (ar - cr, ai - ci), (br + di, bi - dr)]


OWN, Z_IN, Y_IN, ACROSS, ROWS, COLUMNS = range(6)
TUNED = {
    (2, 4, 4, 3, 4): [
        (0, 0, 0), (0, 0, 1), (0, 0, 2), (1, 0, 1, 0), (1, 0, 1, 1), (0, 1, 0), (0, 0, 3), (1, 0, 2, 0),
        (0, 1, 1), (4, 0, 0, 0), (2, 0, 0, 0), (1, 0, 1, 2), (2, 0, 0, 1), (4, 0, 1, 0), (1, 0, 2, 1), (1, 0, 3, 0),
        (1, 0, 2, 2), (0, 1, 2), (1, 1, 1, 0), (2, 0, 2, 0), (4, 0, 2, 0), (2, 0, 1, 0), (1, 0, 3, 1), (1, 0, 3, 2),
        (2, 0, 0, 2), (4, 0, 3, 0), (2, 1, 0, 0), (0, 1, 3), (5, 0, 1, 0, 0), (5, 0, 1, 1, 0), (2, 1, 0, 1), (5, 0, 1, 2, 0),
        (2, 0, 3, 0), (2, 0, 1, 1), (1, 1, 1, 1), (1, 1, 2, 0), (5, 0, 1, 3, 0), (2, 0, 1, 2), (1, 1, 1, 2), (4, 0, 0, 1),
        (2, 0, 2, 1), (4, 1, 0, 0), (3, 1, 0), (4, 0, 1, 1), (2, 0, 3, 1), (1, 1, 2, 1), (5, 0, 0, 0, 0), (2, 0, 2, 2),
        (4, 1, 1, 0), (1, 1, 3, 0), (4, 0, 2, 1), (2, 0, 3, 2), (2, 1, 0, 2), (5, 0, 0, 1, 0), (5, 0, 0, 2, 0), (5, 0, 0, 3, 0),
        (1, 1, 2, 2), (4, 0, 3, 1), (3, 1, 2), (3, 1, 1), (2, 1, 2, 0), (5, 0, 1, 0, 1), (4, 1, 0, 1), (5, 0, 1, 1, 1),
        (5, 0, 1, 2, 1), (2, 1, 1, 0), (5, 0, 1, 3, 1), (5, 0, 0, 0, 1), (1, 1, 3, 1), (5, 0, 0, 1, 1), (5, 0, 0, 2, 1), (4, 1, 2, 0),
        (2, 1, 3, 0), (5, 0, 0, 3, 1), (2, 1, 2, 1), (1, 1, 3, 2), (4, 1, 3, 0), (5, 1, 1, 0, 0), (5, 1, 1, 1, 0), (5, 1, 1, 2, 0),
        (5, 1, 1, 3, 0), (5, 1, 0, 0, 0), (5, 1, 0, 1, 0), (5, 1, 0, 2, 0), (2, 1, 1, 1), (2, 1, 1, 2), (2, 1, 2, 2), (2, 1, 3, 1),
        (4, 1, 1, 1), (5, 1, 0, 3, 0), (4, 1, 2, 1), (2, 1, 3, 2), (4, 1, 3, 1), (5, 1, 1, 0, 1), (5, 1, 1, 1, 1), (5, 1, 1, 2, 1),
        (5, 1, 1, 3, 1), (5, 1, 0, 0, 1), (5, 1, 0, 1, 1), (5, 1, 0, 2, 1), (5, 1, 0, 3, 1),
    ],
}


def program(spc, nz, pieces, parts, radix):
    key = (spc, nz, pieces, len(parts), radix)
    if key in TUNED:
        return TUNED[key]
    order = []
    for l in range(spc):
        order += [(OWN, l, p) for p in range(pieces)]
        end = l == spc - 1
        for j in range(nz):
            order += [(Z_IN, l, j, p) for p in parts if j]
            order += [(Y_IN, l, j, p) for p in parts if not (end and j == 1)]
        order += [(ACROSS, l, p) for p in parts if end]
        order += [(Y_IN, l, 1, p) for p in parts if end]
        order += [(ROWS, l, k, other) for k in range(nz) for other in (0, 1)]
        order += [(COLUMNS, l, tile, rx, phase) for phase in (0, 1) for tile in (1, 0) for rx in range(radix)]
    return order


def kernel(dims, owner_ref, weight_ref, mask_hbm, kern_hbm, rowt_hbm, colt_hbm, out_ref,
           side, held, mask, rowt, colt, lane_perm, stage, field, cols, acc, total, part, blocks,
           loc, k_recv, m_recv, e_recv, z_recv, y_recv, x_recv, p_recv, gone, *kern):
    spc, nk, nz, rows, n, radix = dims
    m = n // radix
    last = spc - 1
    g = lax.axis_index("kgrp")
    t = lax.axis_index("tile")
    x, c = g // 2, g % 2
    z, y = t // 2, t % 2
    xo, co, yo = 1 - x, 1 - c, 1 - y
    x_peer, c_peer = {"kgrp": 2 * xo + c}, {"kgrp": 2 * x + co}
    y_peer = {"tile": 2 * z + yo}

    def at_z(i):
        return {"tile": 2 * i + y}

    unit = 8
    nt = rows // unit
    share = nt // 4
    keep = nt - share
    wide = max(share, 1)
    cuts = [(i, i + wide) for i in range(0, nt, wide)]
    parts = [p for p, cut in enumerate(cuts) if cut[1] <= keep]

    def tiles_of(s, a, b):
        return pl.ds(pl.multiple_of(a * unit + s * (rows - unit * (a + b)), unit), unit * (b - a))

    barrier = pltpu.get_barrier_semaphore()
    for peer in (c_peer, x_peer, y_peer):
        pl.semaphore_signal(barrier, inc=1, device_id=peer, device_id_type=MESH)

    @pl.when(z > 0)
    def _():
        pl.semaphore_signal(barrier, inc=1, device_id=at_z(z - 1), device_id_type=MESH)

    @pl.when(z < nz - 1)
    def _():
        pl.semaphore_signal(barrier, inc=1, device_id=at_z(z + 1), device_id_type=MESH)

    def span(s, p):
        return tiles_of(s, *cuts[p])

    def pieces_of(l, p):
        a, b = cuts[p]
        return [(a, a + 1), (a + 1, b)] if l == p == 0 and b - a > 1 else [(a, b)]

    def candidates(core, p):
        return kern[p].at[pl.ds(core * nk, nk)]

    first_loads = [pltpu.make_async_copy(kern_hbm.at[:, :, span(xo, p)], candidates(c, p), loc.at[3 + p])
                   for p in range(len(cuts))]
    loads = [
        pltpu.make_async_copy(mask_hbm, mask.at[0], loc.at[0]),
        pltpu.make_async_copy(rowt_hbm, rowt, loc.at[1]),
        pltpu.make_async_copy(colt_hbm, colt, loc.at[2]),
    ]
    for load in first_loads + loads:
        load.start()
    for load in first_loads:
        load.wait()
    pl.semaphore_wait(barrier, 3 + jnp.minimum(z, 1) + jnp.minimum(nz - 1 - z, 1))

    groups = {}

    def send(src, dst, recv_sem, device, group, cond=None):
        index, _, size = groups.setdefault(group, (len(groups), cond, 0))
        groups[group] = index, cond, size + math.prod(src.shape) // n
        copy = pltpu.make_async_remote_copy(src_ref=src, dst_ref=dst, send_sem=gone.at[index], recv_sem=recv_sem,
                                            device_id=device, device_id_type=MESH)
        if cond is None:
            copy.start()
        else:
            pl.when(cond)(copy.start)

    def all_gone():
        for index, cond, size in groups.values():
            if size <= n:
                ref = mask.at[0, 0, pl.ds(0, size)]
            elif size <= 2 * n:
                ref = mask.at[0, :, pl.ds(0, size // 2)]
            else:
                ref = mask.at[:, :, pl.ds(0, size // 4)]
            wait = pltpu.make_async_remote_copy(src_ref=ref, dst_ref=ref, send_sem=gone.at[index],
                                                recv_sem=gone.at[index], device_id=c_peer, device_id_type=MESH).wait_send
            if cond is None:
                wait()
            else:
                pl.when(cond)(wait)

    def arrive(ref, recv_sem):
        pltpu.make_async_remote_copy(src_ref=ref, dst_ref=ref, send_sem=recv_sem, recv_sem=recv_sem,
                                     device_id=c_peer, device_id_type=MESH).wait_recv()

    def piece(l, zz, yy, s, p):
        return held.at[l, zz, yy, :, span(s, p)]

    for p in range(len(cuts)):
        src = candidates(c, p)
        send(src, src, k_recv.at[p], c_peer, "core")
    owners = [owner_ref[c * spc + l] for l in range(spc)]
    for p in range(len(cuts)):
        arrive(candidates(co, p), k_recv.at[p])
        for l in range(spc):
            side[x, l, :, span(xo, p)] = kern[p][owners[l] % (2 * nk)]
        for i, sub in enumerate(pieces_of(0, p)):
            src = side.at[x, 0, :, tiles_of(xo, *sub)]
            send(src, src, e_recv.at[0, p + (len(cuts) if i else 0)], x_peer, "core")
    for l in range(1, spc):
        for p in range(len(cuts)):
            src = side.at[x, l, :, span(xo, p)]
            send(src, src, e_recv.at[l, p], x_peer, "core")

    half = n // 2
    wide_lane = m // 2
    src_lane = lax.broadcasted_iota(jnp.int32, (half, half), 0)
    dst_lane = lax.broadcasted_iota(jnp.int32, (half, half), 1)
    perm = jnp.where((src_lane % wide_lane) * radix + src_lane // wide_lane == dst_lane, 1.0, 0.0).astype(BF)
    lane_perm[:half] = perm
    lane_perm[half:] = perm

    def own(l, p):
        mine = owners[l] // (2 * nk) == x
        for i, sub in enumerate(pieces_of(l, p)):
            at = tiles_of(x, *sub)
            arrive(side.at[xo, l, :, at], e_recv.at[l, p + (len(cuts) if i else 0)])
            held[l, z, y, :, at] = jnp.where(mine, side[x, l, :, at], side[xo, l, :, at])
            if p in parts:
                here = held.at[l, z, y, :, at]
                send(here, here, y_recv.at[l, z, p], y_peer, "core")
                send(here, here, z_recv.at[l, z, p], at_z(z - 1), "down", z > 0)
                send(here, here, z_recv.at[l, z, p], at_z(z + 1), "up", z < nz - 1)

    def across(l, p):
        here = piece(l, z, yo, x, p)
        send(here, here, y_recv.at[l, z, p], at_z(z - 1), "down", z > 0)
        send(here, here, y_recv.at[l, z, p], at_z(z + 1), "up", z < nz - 1)

    def share_x(l, zz, yy, group, cond=None):
        if share:
            here = piece(l, zz, yy, x, 0)
            send(here, here, x_recv.at[l, zz, yy], x_peer, group, cond)

    def z_in(l, j, p):
        for s, zz, have, dest, more in ((1, z + j, z + j < nz, z - 1, z > 0), (-1, z - j, z >= j, z + 1, z < nz - 1)):
            here = piece(l, zz, y, x, p)
            pl.when(have)(functools.partial(arrive, here, z_recv.at[l, zz, p]))
            if j < nz - 1:
                send(here, here, z_recv.at[l, zz, p], at_z(dest), ("relay", s * j), have & more)
            if l != last or j > 1:
                send(here, here, y_recv.at[l, zz, p], y_peer, ("on", s * j), have)
            if p == 0:
                share_x(l, zz, y, ("on", s * j), have)

    def y_in(l, j, p):
        if j == 0:
            arrive(piece(l, z, yo, x, p), y_recv.at[l, z, p])
            if p == 0:
                share_x(l, z, yo, "core")
            return
        for s, zz, have in ((1, z + j, z + j < nz), (-1, z - j, z >= j)):
            pl.when(have)(functools.partial(arrive, piece(l, zz, yo, x, p), y_recv.at[l, zz, p]))
            if p == 0:
                share_x(l, zz, yo, ("on", s * j), have)

    def near(k):
        if k == 0:
            return z
        low = jnp.minimum(z, nz - 1 - z)
        both = z + (k + 1) // 2 if k % 2 else z - k // 2
        one = jnp.where(low == z, z + k - low, z - k + low)
        return jnp.where(k <= 2 * low, both, one)

    def x_in(l, k, yy):
        if share and not (k == 0 and yy is y):
            arrive(piece(l, near(k), yy, xo, 0), x_recv.at[l, near(k), yy])

    strip = 16
    waiting = []

    def product(l, k, yy, slot, tile, strip_index):
        zi = near(k)
        lo_row = strip * strip_index
        at = pl.ds(pl.multiple_of((2 * zi + yy) * rows + lo_row, strip), strip)
        src = slice(lo_row, lo_row + strip)
        to = slice(tile * rows + lo_row, tile * rows + lo_row + strip)
        re, im = [], []
        for q in range(radix):
            lanes = slice(q * m, (q + 1) * m)
            kr, ki = held[l, zi, yy, 0, src, lanes], held[l, zi, yy, 1, src, lanes]
            mr, mi = mask[tile, 0, at, lanes], mask[tile, 1, at, lanes]
            re.append(mr * kr - mi * ki)
            im.append(mr * ki + mi * kr)
        for r, pair in enumerate(radix4(re, im)):
            for p, v in enumerate(pair):
                hi, lo = split(v)
                stage[slot, r, to, p * m:(p + 1) * m] = hi
                stage[slot, r, to, (2 + p) * m:(3 + p) * m] = lo

    def row_matmul(l, k, yy, slot, r):
        hi, lo = stage[slot, r, :, :2 * m], stage[slot, r, :, 2 * m:]
        th, tl = rowt[r, :2 * m], rowt[r, 2 * m:]
        done = jnp.dot(jnp.concatenate([hi, lo, hi], 1), jnp.concatenate([th, th, tl], 0),
                       preferred_element_type=F32)
        at = pl.ds(pl.multiple_of((2 * near(k) + yy) * rows, rows), rows)
        for tile in range(2):
            field[l, r, tile, at] = done[tile * rows:(tile + 1) * rows]

    def woven(first, second):
        count = max(len(first), len(second))
        for i in range(count):
            for group in (first, second):
                for work in group[i * len(group) // count:(i + 1) * len(group) // count]:
                    work()

    def held_matmuls():
        works = [functools.partial(row_matmul, *waiting[0], r) for r in range(radix)] if waiting else []
        waiting.clear()
        return works

    def row_step(l, k, other):
        yy = yo if other else y
        x_in(l, k, yy)
        slot = 1 - waiting[0][3] if waiting else 0
        products = [functools.partial(product, l, k, yy, slot, tile, i)
                    for i in range(rows // strip) for tile in range(2)]
        woven(held_matmuls(), products)
        waiting.append((l, k, yy, slot))

    def middle(l, tile, ry, phase):
        own_half = y if phase == 0 else yo

        def strip_of(i):
            at = strip * i
            base = at // rows * 2 * rows + at % rows
            lanes = slice(ry * m, (ry + 1) * m)
            from_rows = [pl.ds(pl.multiple_of(k * m + base + own_half * rows, strip), strip) for k in range(radix)]
            re = [field[l, ry, tile, rows_at, :m] for rows_at in from_rows]
            im = [field[l, ry, tile, rows_at, m:] for rows_at in from_rows]
            for rx, pair in enumerate(radix4(re, im)):
                for p, v in enumerate(pair):
                    hi, lo = split(v)
                    to = p * (m // 2) + at
                    cols[tile, rx, to:to + strip, lanes] = hi
                    cols[tile, rx, m + to:m + to + strip, lanes] = lo
        return [functools.partial(strip_of, i) for i in range(m // 2 // strip)]

    def columns(l, tile, rx, phase):
        hi, lo = cols[tile, rx, :m], cols[tile, rx, m:]
        own_half = y if phase == 0 else yo
        th, tl = colt[rx, own_half, :, :m], colt[rx, own_half, :, m:]
        done = (jnp.dot(jnp.concatenate([th, tl], 1), jnp.concatenate([hi, hi], 0), preferred_element_type=F32)
                + jnp.dot(th, lo, preferred_element_type=F32))
        if phase == 0:
            acc[tile, rx] = done
            return
        done += acc[tile, rx]
        power = (done[:m] * done[:m] + done[m:] * done[m:]) * weight_ref[c * spc + l]
        if l == 0:
            total[tile, rx] = power
        else:
            total[tile, rx] += power

    def column_step(l, tile, rx, phase):
        if rx == 0 and waiting and waiting[0][0] == l:
            woven(held_matmuls(), [])
        if rx == 0 and tile == 1:
            for ry in range(radix):
                woven(middle(l, tile, ry, phase), [])
        woven([functools.partial(columns, l, tile, rx, phase)], middle(l, 0, rx, phase) if tile == 1 else [])
        if l == last and tile == 1 and phase == 1:
            for done in [rx - 1] if rx < radix - 1 else [rx - 1, rx]:
                if done >= 0:
                    send(total.at[1, done], part.at[done], p_recv.at[0], c_peer, "part")

    steps = (own, z_in, y_in, across, row_step, column_step)
    first_row = mask_unsent = True
    for op, *args in program(spc, nz, len(cuts), parts, radix):
        if op == 4 and first_row:
            first_row = False
            for load in loads:
                load.wait()
            arrive(mask.at[1], m_recv.at[0])
        steps[op](*args)
        if mask_unsent and (op, *args) == (OWN, 0, min(1, len(cuts) - 1)):
            mask_unsent = False
            send(mask_hbm, mask.at[1], m_recv.at[0], c_peer, "mask")

    arrive(part, p_recv.at[0])
    low = lax.broadcasted_iota(jnp.int32, (m, m), 1) < wide_lane
    perm = lane_perm[...]
    for rx in range(radix):
        lanes = [total[0, rx, :, r * m:(r + 1) * m] + part[rx, :, r * m:(r + 1) * m] for r in range(radix)]
        turned = [pltpu.roll(v, wide_lane, 1) for v in lanes]
        for h in range(2):
            pairs = [jnp.where(low, *((lanes[r], turned[r + 1]) if h == 0 else (turned[r], lanes[r + 1])))
                     for r in range(0, radix, 2)]
            hi, lo = split(jnp.concatenate(pairs, 1))
            image = jnp.dot(jnp.concatenate([hi, lo], 1), perm, preferred_element_type=F32)
            for q in range(radix // 2):
                blocks[h * (radix // 2) + q, pl.ds(rx, m, stride=radix), :] = image[:, q * m:(q + 1) * m]
    for q in range(radix):
        out_ref[:, q * m:(q + 1) * m] = blocks[q]
    all_gone()


def local(mesh_shape, mask_spectrum, kernels, owner_table, step_weight):
    groups, tiles = mesh_shape
    nk, _, rows, n = kernels.shape
    steps = owner_table.shape[0]
    radix = 4
    m = n // radix
    spc = steps // 2
    nz = tiles // 2
    most = min(rows // 8, 4)
    kept = most - (rows // 8 >= 4)
    rowt, colt = tables(n, radix, rows)
    dma = pltpu.SemaphoreType.DMA
    any_spec = pl.BlockSpec(memory_space=pl.ANY)
    smem = pl.BlockSpec(memory_space=pltpu.SMEM)
    out = pl.pallas_call(
        functools.partial(kernel, (spc, nk, nz, rows, n, radix)),
        out_shape=pltpu.VMEM((n, n), F32),
        in_specs=[smem, smem, any_spec, any_spec, any_spec, any_spec],
        out_specs=pl.BlockSpec(memory_space=pltpu.VMEM),
        scratch_shapes=[
            pltpu.VMEM((2, spc, 2, rows, n), F32),
            pltpu.VMEM((spc, nz, 2, 2, rows, n), F32),
            pltpu.VMEM((2, 2, n, n), F32),
            pltpu.VMEM(rowt.shape, BF),
            pltpu.VMEM(colt.shape, BF),
            pltpu.VMEM((n, n // 2), BF),
            pltpu.VMEM((2, radix, 2 * rows, 4 * m), BF),
            pltpu.VMEM((spc, radix, 2, n, 2 * m), F32),
            pltpu.VMEM((2, radix, 2 * m, n), BF),
            pltpu.VMEM((2, radix, 2 * m, n), F32),
            pltpu.VMEM((2, radix, m, n), F32),
            pltpu.VMEM((radix, m, n), F32),
            pltpu.VMEM((radix, n, m), F32),
            dma((3 + most,)), dma((most,)), dma((1,)), dma((spc, most + 1)), dma((spc, nz, kept)), dma((spc, nz, kept)),
            dma((spc, nz, 2)), dma((1,)), dma((4 * nz - 1,)),
        ] + [pltpu.VMEM((2 * nk, 2, rows // most, n), F32)] * most,
        compiler_params=pltpu.CompilerParams(collective_id=0, has_side_effects=True, vmem_limit_bytes=54 * 1024 * 1024),
    )(owner_table, step_weight, mask_spectrum[0], kernels, jnp.asarray(rowt), jnp.asarray(colt))
    return out[None]


def solution(mesh):
    in_specs = (P(("kgrp", "tile"), None, None, None), P("kgrp", None, "tile", None), P(), P())
    out_specs = P(("kgrp", "tile"), None, None)
    body = functools.partial(local, (mesh.shape["kgrp"], mesh.shape["tile"]))
    return jax.shard_map(body, mesh=mesh, in_specs=in_specs, out_specs=out_specs, check_vma=False)
```
